256 devices in a mesh: chain: 256 (over y, x, z, core).
Axes of the slice: x: 4, y: 4, z: 8, core: 2. Of those that a mesh axis runs over, the one named last changes fastest.
Arguments:
- right_side: float32 [8, 32768], P(None, 'chain'), may hold values from -6 to 6
- diag_block: float32 [8, 8, 32768], P(None, None, 'chain'), may hold values from -2 to 2
- below_block: float32 [8, 8, 32768], P(None, None, 'chain'), may hold values from -2 to 2
- above_block: float32 [8, 8, 32768], P(None, None, 'chain'), may hold values from -2 to 2
- lower_level: float32 [15, 8, 8, 32768], P(None, None, None, 'chain'), may hold values from -0.5 to 0.5
- upper_level: float32 [15, 8, 8, 32768], P(None, None, None, 'chain'), may hold values from -0.5 to 0.5
- final_block: float32 [8, 8, 32768], P(None, None, 'chain'), may hold values from -1 to 1
Outputs:
- basis: float32 [4, 8, 32768], P(None, None, 'chain')
- hess: float32 [4, 3], replicated
The draws below stay inside these ranges and needn't reach their ends.
All inputs are finite; a program needn't handle non-finite values.
Results may differ from the reference program's by a relative error of at most 0.0001.
Values sent between devices are 32-bit elements; how exact they have to be, the bound alone decides.
A program may use at most 64 MiB of HBM per device.

```python
import jax
import jax.numpy as jnp
from jax import lax

BLK = 8
ITERS = 3
NB = 32768
LEVELS = 15


def level_of(stream_key, extent, shards, least, high):
    gain = 1.0
    for position, blocks in shards:
        steps = jax.random.uniform(jax.random.fold_in(jax.random.fold_in(stream_key, 6), position), (blocks,), jnp.float32, least / len(shards), high / len(shards))
        gain = gain * jnp.repeat(jnp.exp(steps), extent[position] // blocks).reshape((-1,) + (1,) * (len(extent) - 1 - position))
    return gain


def noise(rng, extent, scale, reach, shards=(), kind=jnp.bfloat16):
    level = level_of(rng, extent, shards, -0.22, 0.18) if shards else 1.0
    entries = jax.random.normal(rng, extent, jnp.float32) * scale * level
    return jnp.minimum(jnp.maximum(entries, -reach), reach).astype(kind)


def setup_inputs(seed: int = 0) -> dict:
    streams_of = jax.random.split(jax.random.key(seed), 8)
    return {
        "right_side": noise(streams_of[0], (BLK, NB), 1.0, 6.0, ((1, 256),), jnp.float32),
        "diag_block": noise(streams_of[1], (BLK, BLK, NB), BLK ** -0.5, 2.0, ((2, 256),), jnp.float32),
        "below_block": noise(streams_of[2], (BLK, BLK, NB), BLK ** -0.5, 2.0, ((2, 256),), jnp.float32),
        "above_block": noise(streams_of[3], (BLK, BLK, NB), BLK ** -0.5, 2.0, ((2, 256),), jnp.float32),
        "lower_level": noise(streams_of[4], (LEVELS, BLK, BLK, NB), (16 * BLK) ** -0.5, 0.5, ((3, 256),), jnp.float32),
        "upper_level": noise(streams_of[5], (LEVELS, BLK, BLK, NB), (16 * BLK) ** -0.5, 0.5, ((3, 256),), jnp.float32),
        "final_block": noise(streams_of[6], (BLK, BLK, NB), (4 * BLK) ** -0.5, 1.0, ((2, 256),), jnp.float32),
    }


EPS = 1e-06

def blockmul(blocks, field):
    return jnp.einsum('abi,bi->ai', blocks, field, precision=lax.Precision.HIGHEST)

def lower_shift(field, stride):
    total = field.shape[1]
    if stride >= total:
        return jnp.zeros_like(field)
    return jnp.pad(field, ((0, 0), (stride, 0)))[:, :total]

def upper_shift(field, stride):
    total = field.shape[1]
    if stride >= total:
        return jnp.zeros_like(field)
    return jnp.pad(field, ((0, 0), (0, stride)))[:, stride:]

def operate(field, diag_block, below_block, above_block):
    result = 2.0 * field + blockmul(diag_block, field)
    result = result + blockmul(below_block, lower_shift(field, 1))
    return result + blockmul(above_block, upper_shift(field, 1))

def precondition(field, lower_level, upper_level, final_block):
    for level in range(lower_level.shape[0]):
        stride = 2 ** level
        field = field + blockmul(lower_level[level], lower_shift(field, stride)) + blockmul(upper_level[level], upper_shift(field, stride))
    return field + blockmul(final_block, field)

def reference(right_side, diag_block, below_block, above_block, lower_level, upper_level, final_block):
    count = right_side.shape[0] * right_side.shape[1]
    start = right_side / jnp.sqrt(jnp.sum(right_side * right_side) / count + EPS)
    basis = [start]
    hess = jnp.zeros((ITERS + 1, ITERS), jnp.float32)
    for column in range(ITERS):
        vector = operate(precondition(basis[column], lower_level, upper_level, final_block), diag_block, below_block, above_block)
        stacked = jnp.stack(basis)
        dots = jnp.einsum('kai,ai->k', stacked, vector, precision=lax.Precision.HIGHEST) / count
        vector = vector - jnp.einsum('k,kai->ai', dots, stacked, precision=lax.Precision.HIGHEST)
        length = jnp.sqrt(jnp.sum(vector * vector) / count + EPS)
        basis.append(vector / length)
        hess = hess.at[:column + 1, column].set(dots).at[column + 1, column].set(length)
    return (jnp.stack(basis), hess)
```

```python
import functools

import jax
import jax.numpy as jnp
from jax import lax
from jax.experimental import pallas as pl
from jax.experimental.pallas import tpu as pltpu
from jax.sharding import PartitionSpec as P

ITERS = 3
EPS = 1e-06
DEV = 256
ROWS = 128
COUNT = 8 * DEV * ROWS
F32 = jnp.float32
NEAR = 7
LOWS = (-3, -2, -1, 1, 2, 3)


def kernel(
    r_hbm, dg_hbm, bl_hbm, ab_hbm, lo_hbm, up_hbm, fb_hbm,
    basis_ref, hess_ref,
    rv, av, fv, cf,
    near_c, near_a, c7, c9, c11, c12, c13,
    xs, bs, gr,
    src1, src2, src3, srct, srcz, srcp,
    h1, h2, h3, ht, hz, hp,
    lsem, msend, mrecv, rsend, rrecv,
):
    d = lax.axis_index("chain")
    t = lax.rem(d, 16)
    line = d - t

    def dev(offset):
        return lax.rem(d + (offset % DEV), DEV)

    def in_line(offset):
        return line + lax.rem(t + (offset % 16), 16)

    loads = [
        pltpu.make_async_copy(r_hbm, rv, lsem.at[0]),
        pltpu.make_async_copy(lo_hbm, cf.at[:, 0], lsem.at[1]),
        pltpu.make_async_copy(up_hbm, cf.at[:, 1], lsem.at[2]),
        pltpu.make_async_copy(dg_hbm, av.at[0], lsem.at[3]),
        pltpu.make_async_copy(bl_hbm, av.at[1], lsem.at[4]),
        pltpu.make_async_copy(ab_hbm, av.at[2], lsem.at[5]),
        pltpu.make_async_copy(fb_hbm, fv, lsem.at[6]),
    ]
    for load in loads:
        load.start()

    partners = [dev(o) for o in (-12, -8, -4, -3, -2, -1, 1, 2, 3, 4, 8, 12)]
    partners += [dev(16 * o) for o in range(1, 16)]
    partners += [in_line(o) for o in range(1, 16)]
    barrier = pltpu.get_barrier_semaphore()
    for other in partners:
        pl.semaphore_signal(barrier, inc=1, device_id=(other,), device_id_type=pl.DeviceIdType.MESH)
    pl.semaphore_wait(barrier, len(partners))

    def send(src, dst, ssem, rsem, other):
        pltpu.make_async_remote_copy(
            src_ref=src, dst_ref=dst, send_sem=ssem, recv_sem=rsem,
            device_id=(other,), device_id_type=pl.DeviceIdType.MESH,
        ).start()

    def drain(buf, sem):
        pltpu.make_async_copy(buf, buf, sem).wait()

    for load in loads:
        load.wait()

    send(rv, h1.at[0, 1], rsend.at[0, 0], rrecv.at[0, 0], dev(-1))
    send(rv, h1.at[0, 0], rsend.at[0, 0], rrecv.at[0, 0], dev(1))
    send(cf.at[pl.ds(0, 6)], near_c.at[1], msend.at[0], mrecv.at[0], dev(-1))
    send(cf.at[pl.ds(0, 6)], near_c.at[0], msend.at[0], mrecv.at[0], dev(1))
    send(cf.at[7], c7.at[1], msend.at[1], mrecv.at[1], dev(-2))
    send(cf.at[7], c7.at[0], msend.at[1], mrecv.at[1], dev(2))
    send(cf.at[9], c9.at[1], msend.at[2], mrecv.at[2], dev(-8))
    send(cf.at[9], c9.at[0], msend.at[2], mrecv.at[2], dev(8))
    for p in range(2, 16, 2):
        send(cf.at[11], c11.at[p // 2 - 1], msend.at[3], mrecv.at[3], dev(-16 * p))
    for p in range(4, 16, 4):
        send(cf.at[12], c12.at[p // 4 - 1], msend.at[4], mrecv.at[4], dev(-16 * p))
    send(cf.at[13], c13, msend.at[5], mrecv.at[5], dev(-16 * 8))
    send(av, near_a.at[1], msend.at[6], mrecv.at[6], dev(-1))
    send(av, near_a.at[0], msend.at[6], mrecv.at[6], dev(1))

    lane = lax.broadcasted_iota(jnp.int32, (8, ROWS), 1)
    sub = lax.broadcasted_iota(jnp.int32, (8, ROWS), 0)

    def flag(cond):
        return jnp.where(cond, 1.0, 0.0).astype(F32)

    has_below, has_above = flag(d >= 1), flag(d <= DEV - 2)

    def mul(blocks, v):
        total = blocks[pl.ds(0, 8, stride=8), :] * v[0:1]
        for b in range(1, 8):
            total = total + blocks[pl.ds(b, 8, stride=8), :] * v[b : b + 1]
        return total

    def step(coef, x, below, above):
        return x + mul(coef.at[0], below) + mul(coef.at[1], above)

    def down(u, prev, s):
        return jnp.where(lane < s, pltpu.roll(prev, s, 1), pltpu.roll(u, s, 1))

    def upward(u, following, s):
        return jnp.where(
            lane >= ROWS - s, pltpu.roll(following, ROWS - s, 1), pltpu.roll(u, ROWS - s, 1)
        )

    def far_level(coef, x, below, above, p, by, scale=1, size=DEV):
        place = lax.rem(d + (p % DEV), DEV)
        return step(
            coef, x, below * flag(place >= by), above * flag(place + by <= DEV - 1)
        )

    def send_sums(block, j):
        srcz[j] = block
        for o in range(1, 16):
            send(srcz.at[j], hz.at[j, o - 1], rsend.at[j, 4], rrecv.at[j, 4], in_line(-o))

    def pass_sums(j):
        drain(hz.at[j], rrecv.at[j, 4])
        total = srcz[j]
        for o in range(15):
            total = total + hz[j, o]
        srcp[j] = total
        for o in range(1, 16):
            send(srcp.at[j], hp.at[j, o - 1], rsend.at[j, 5], rrecv.at[j, 5], dev(-16 * o))

    def take_sums(j):
        drain(hp.at[j], rrecv.at[j, 5])
        total = srcp[j]
        for o in range(15):
            total = total + hp[j, o]
        return jnp.sum(total, axis=1, keepdims=True) * (1.0 / COUNT) + jnp.zeros((8, ROWS), F32)

    def finish(j, x, hess):
        sums = take_sums(j)
        h = [sums[i : i + 1] for i in range(3)]
        squares = sums[3:4]
        gr[lax.max(j - 1, 0)] = sums
        for i in range(3):
            squares = squares - 2.0 * (h[i] * h[i])
        for c in range(3):
            g = gr[c]
            for i in range(c + 1):
                squares = squares + (1.0 if i == c else 2.0) * (h[c] * h[i]) * g[4 + i : 5 + i]
        length = jnp.sqrt(jnp.maximum(squares, 0.0) + EPS)
        inverse = 1.0 / length
        new = x
        for i in range(3):
            new = new - h[i] * bs[i]
        new = new * inverse
        column = jnp.where(sub < 3, sums, 0.0)
        column = jnp.where(sub == j, length + jnp.zeros((8, ROWS), F32), column)
        hess = jnp.where(lane == j - 1, column, hess)
        return h, inverse, new, hess

    zero = jnp.zeros((8, ROWS), F32)
    for i in range(4):
        bs[i] = zero
    for i in range(3):
        gr[i] = zero
    for i in range(4):
        for c in range(3):
            xs[i, c] = zero

    r = rv[...]
    send_sums(jnp.where(sub == 3, jnp.sum(r * r, axis=0, keepdims=True) + zero, 0.0), 0)
    drain(h1.at[0], rrecv.at[0, 0])
    xs[0, 0] = h1[0, 0] * has_below
    xs[0, 1] = r
    xs[0, 2] = h1[0, 1] * has_above
    drain(near_c, mrecv.at[0])

    def body(j, hess):
        u = [xs[j, 0], xs[j, 1], xs[j, 2]]
        for level in range(NEAR):
            s = 2**level
            mid = step(cf.at[level], u[1], down(u[1], u[0], s), upward(u[1], u[2], s))
            if level < NEAR - 1:
                left = step(
                    near_c.at[0, level], u[0], down(u[0], u[0], s), upward(u[0], u[1], s)
                ) * has_below
                right = step(
                    near_c.at[1, level], u[2], down(u[2], u[1], s), upward(u[2], u[2], s)
                ) * has_above
                u = [left, mid, right]
            else:
                u = [None, mid, None]
        x = u[1]

        def group(x, src, got, slot, near_coef, level, by):
            src[j] = x
            for k, o in enumerate(LOWS):
                send(src.at[j], got.at[j, k], rsend.at[j, slot], rrecv.at[j, slot], dev(-o * by))
            drain(got.at[j], rrecv.at[j, slot])
            f = {o: got[j, k] for k, o in enumerate(LOWS)}
            f[0] = x
            y = {
                0: far_level(cf.at[level], f[0], f[-1], f[1], 0, by),
                -2: far_level(near_coef.at[0], f[-2], f[-3], f[-1], -2 * by, by),
                2: far_level(near_coef.at[1], f[2], f[1], f[3], 2 * by, by),
            }
            return far_level(cf.at[level + 1], y[0], y[-2], y[2], 0, 2 * by)

        @pl.when(j == 0)
        def _():
            drain(c7, mrecv.at[1])

        x = group(x, src2, h2, 1, c7, 7, 1)

        @pl.when(j == 0)
        def _():
            drain(c9, mrecv.at[2])

        x = group(x, src3, h3, 2, c9, 9, 4)

        srct[j] = x
        for o in range(1, 16):
            send(srct.at[j], ht.at[j, o - 1], rsend.at[j, 3], rrecv.at[j, 3], dev(-16 * o))
        pass_sums(j)

        @pl.when(j == 0)
        def _():
            drain(c11, mrecv.at[3])
            drain(c12, mrecv.at[4])
            drain(c13, mrecv.at[5])

        drain(ht.at[j], rrecv.at[j, 3])
        f = [x] + [ht[j, o] for o in range(15)]

        def top(coef, field, p, by):
            return far_level(
                coef, field[p], field[(p - by) % 16], field[(p + by) % 16], 16 * p, 16 * by
            )

        y1 = {p: top(cf.at[11] if p == 0 else c11.at[p // 2 - 1], f, p, 1) for p in range(0, 16, 2)}
        y2 = {p: top(cf.at[12] if p == 0 else c12.at[p // 4 - 1], y1, p, 2) for p in range(0, 16, 4)}
        y3 = {p: top(cf.at[13] if p == 0 else c13, y2, p, 4) for p in (0, 8)}
        x = top(cf.at[14], y3, 0, 8)
        x = x + mul(fv, x)

        src1[j] = x
        send(src1.at[j], h1.at[j + 1, 1], rsend.at[j + 1, 0], rrecv.at[j + 1, 0], dev(-1))
        send(src1.at[j], h1.at[j + 1, 0], rsend.at[j + 1, 0], rrecv.at[j + 1, 0], dev(1))

        h, inverse, new, hess = finish(j, xs[j, 1], hess)
        bs[j] = new
        basis_ref[j] = new

        @pl.when(j == 0)
        def _():
            drain(near_a, mrecv.at[6])

        drain(h1.at[j + 1], rrecv.at[j + 1, 0])
        cols = [h1[j + 1, 0] * has_below, x, h1[j + 1, 1] * has_above]
        for c, (coef, mask) in enumerate(
            ((near_a.at[0], has_below), (av, None), (near_a.at[1], has_above))
        ):
            v = 2.0 * cols[c] + mul(coef.at[0], cols[c])
            v = v + mul(coef.at[1], down(cols[c], cols[max(c - 1, 0)], 1))
            v = v + mul(coef.at[2], upward(cols[c], cols[min(c + 1, 2)], 1))
            for i in range(2):
                v = v - h[i] * xs[i + 1, c]
            v = v * inverse
            xs[j + 1, c] = v if mask is None else v * mask

        w = xs[j + 1, 1]
        sums = zero
        rows = [bs[0] * w, bs[1] * w, bs[2] * w, w * w, bs[0] * new, bs[1] * new, bs[2] * new]
        for i, row in enumerate(rows):
            sums = jnp.where(sub == i, jnp.sum(row, axis=0, keepdims=True) + zero, sums)
        send_sums(sums, j + 1)
        return hess

    hess = lax.fori_loop(0, ITERS, body, zero)
    pass_sums(ITERS)
    _, _, new, hess = finish(ITERS, xs[ITERS, 1], hess)
    basis_ref[ITERS] = new
    hess_ref[...] = hess

    drain(near_c, msend.at[0])
    drain(c7, msend.at[1])
    drain(c9, msend.at[2])
    drain(c11, msend.at[3])
    drain(c12, msend.at[4])
    drain(c13, msend.at[5])
    drain(near_a, msend.at[6])
    for j in range(ITERS + 1):
        drain(h1.at[j], rsend.at[j, 0])
        drain(hz.at[j], rsend.at[j, 4])
        drain(hp.at[j], rsend.at[j, 5])
        if j < ITERS:
            drain(h2.at[j], rsend.at[j, 1])
            drain(h3.at[j], rsend.at[j, 2])
            drain(ht.at[j], rsend.at[j, 3])


def on_device(right_side, diag_block, below_block, above_block, lower_level, upper_level, final_block):
    block = (64, ROWS)
    tile = (8, ROWS)
    vmem = lambda *lead: pltpu.VMEM(lead, F32)
    basis, hess = pl.pallas_call(
        kernel,
        out_shape=(
            jax.ShapeDtypeStruct((ITERS + 1, 8, ROWS), F32),
            jax.ShapeDtypeStruct(tile, F32),
        ),
        in_specs=[pl.BlockSpec(memory_space=pl.ANY)] * 7,
        out_specs=(pl.BlockSpec(memory_space=pltpu.VMEM), pl.BlockSpec(memory_space=pltpu.VMEM)),
        scratch_shapes=[
            vmem(*tile), vmem(3, *block), vmem(*block), vmem(15, 2, *block),
            vmem(2, 6, 2, *block), vmem(2, 3, *block), vmem(2, 2, *block), vmem(2, 2, *block),
            vmem(7, 2, *block), vmem(3, 2, *block), vmem(2, *block),
            vmem(4, 3, *tile), vmem(4, *tile), vmem(3, *tile),
            vmem(3, *tile), vmem(3, *tile), vmem(3, *tile), vmem(3, *tile),
            vmem(4, *tile), vmem(4, *tile),
            vmem(4, 2, *tile), vmem(3, 6, *tile), vmem(3, 6, *tile), vmem(3, 15, *tile),
            vmem(4, 15, *tile), vmem(4, 15, *tile),
            pltpu.SemaphoreType.DMA((7,)),
            pltpu.SemaphoreType.DMA((7,)),
            pltpu.SemaphoreType.DMA((7,)),
            pltpu.SemaphoreType.DMA((4, 6)),
            pltpu.SemaphoreType.DMA((4, 6)),
        ],
        compiler_params=pltpu.CompilerParams(collective_id=0, has_side_effects=True),
    )(
        right_side,
        diag_block.reshape(block),
        below_block.reshape(block),
        above_block.reshape(block),
        lower_level.reshape((15,) + block),
        upper_level.reshape((15,) + block),
        final_block.reshape(block),
    )
    return basis, hess[: ITERS + 1, :ITERS]


def solution(mesh):
    blocks = P(None, None, "chain")
    levels = P(None, None, None, "chain")
    return jax.shard_map(
        on_device,
        mesh=mesh,
        in_specs=(P(None, "chain"), blocks, blocks, blocks, levels, levels, blocks),
        out_specs=(P(None, None, "chain"), P()),
        check_vma=False,
    )
```

```python
import functools

import jax
import jax.numpy as jnp
from jax import lax
from jax.experimental import pallas as pl
from jax.experimental.pallas import tpu as pltpu
from jax.sharding import PartitionSpec as P

ITERS = 3
EPS = 1e-06
DEV = 256
ROWS = 128
COUNT = 8 * DEV * ROWS
F32 = jnp.float32
NEAR = 7
LOWS = (-3, -2, -1, 1, 2, 3)


def kernel(
    r_hbm, dg_hbm, bl_hbm, ab_hbm, lo_hbm, up_hbm, fb_hbm,
    basis_ref, hess_ref,
    rv, av, fv, cf,
    near_c, near_a, c7, c9, c11, c12, c13,
    xs, bs, gr,
    src1, src2, src3, srct, srcz, srcp,
    h1, h2, h3, ht, hz, hp,
    lsem, msend, mrecv, rsend, rrecv,
):
    d = lax.axis_index("chain")
    t = lax.rem(d, 16)
    line = d - t

    def dev(offset):
        return lax.rem(d + (offset % DEV), DEV)

    def in_line(offset):
        return line + lax.rem(t + (offset % 16), 16)

    loads = [
        pltpu.make_async_copy(r_hbm, rv, lsem.at[0]),
        pltpu.make_async_copy(lo_hbm, cf.at[:, 0], lsem.at[1]),
        pltpu.make_async_copy(up_hbm, cf.at[:, 1], lsem.at[2]),
        pltpu.make_async_copy(dg_hbm, av.at[0], lsem.at[3]),
        pltpu.make_async_copy(bl_hbm, av.at[1], lsem.at[4]),
        pltpu.make_async_copy(ab_hbm, av.at[2], lsem.at[5]),
        pltpu.make_async_copy(fb_hbm, fv, lsem.at[6]),
    ]
    for load in loads:
        load.start()

    partners = [dev(o) for o in (-12, -8, -4, -3, -2, -1, 1, 2, 3, 4, 8, 12)]
    partners += [dev(16 * o) for o in range(1, 16)]
    partners += [in_line(o) for o in range(1, 16)]
    barrier = pltpu.get_barrier_semaphore()
    for other in partners:
        pl.semaphore_signal(barrier, inc=1, device_id=(other,), device_id_type=pl.DeviceIdType.MESH)
    pl.semaphore_wait(barrier, len(partners))

    def send(src, dst, ssem, rsem, other):
        pltpu.make_async_remote_copy(
            src_ref=src, dst_ref=dst, send_sem=ssem, recv_sem=rsem,
            device_id=(other,), device_id_type=pl.DeviceIdType.MESH,
        ).start()

    def drain(buf, sem):
        pltpu.make_async_copy(buf, buf, sem).wait()

    for load in loads:
        load.wait()

    send(rv, h1.at[0, 1], rsend.at[0, 0], rrecv.at[0, 0], dev(-1))
    send(rv, h1.at[0, 0], rsend.at[0, 0], rrecv.at[0, 0], dev(1))
    send(cf.at[pl.ds(0, 6)], near_c.at[1], msend.at[0], mrecv.at[0], dev(-1))
    send(cf.at[pl.ds(0, 6)], near_c.at[0], msend.at[0], mrecv.at[0], dev(1))

    def send_low(first):
        if first:
            send(cf.at[7], c7.at[1], msend.at[1], mrecv.at[1], dev(-2))
            send(cf.at[7], c7.at[0], msend.at[1], mrecv.at[1], dev(2))
        else:
            send(cf.at[9], c9.at[1], msend.at[2], mrecv.at[2], dev(-8))
            send(cf.at[9], c9.at[0], msend.at[2], mrecv.at[2], dev(8))

    def send_top():
        for p in range(2, 16, 2):
            send(cf.at[11], c11.at[p // 2 - 1], msend.at[3], mrecv.at[3], dev(-16 * p))
        for p in range(4, 16, 4):
            send(cf.at[12], c12.at[p // 4 - 1], msend.at[4], mrecv.at[4], dev(-16 * p))
        send(cf.at[13], c13, msend.at[5], mrecv.at[5], dev(-16 * 8))

    def send_operator():
        send(av, near_a.at[1], msend.at[6], mrecv.at[6], dev(-1))
        send(av, near_a.at[0], msend.at[6], mrecv.at[6], dev(1))

    send_low(True)

    lane = lax.broadcasted_iota(jnp.int32, (8, ROWS), 1)
    sub = lax.broadcasted_iota(jnp.int32, (8, ROWS), 0)
    mine = (lane >= 16 * sub) & (lane < 16 * sub + 16)

    def flag(cond):
        return jnp.where(cond, 1.0, 0.0).astype(F32)

    has_below, has_above = flag(d >= 1), flag(d <= DEV - 2)

    def mul(blocks, v):
        total = blocks[pl.ds(0, 8, stride=8), :] * v[0:1]
        for b in range(1, 8):
            total = total + blocks[pl.ds(b, 8, stride=8), :] * v[b : b + 1]
        return total

    def step(coef, x, below, above):
        return x + mul(coef.at[0], below) + mul(coef.at[1], above)

    def down(u, prev, s):
        return jnp.where(lane < s, pltpu.roll(prev, s, 1), pltpu.roll(u, s, 1))

    def upward(u, following, s):
        return jnp.where(
            lane >= ROWS - s, pltpu.roll(following, ROWS - s, 1), pltpu.roll(u, ROWS - s, 1)
        )

    def far_level(coef, x, below, above, p, by, scale=1, size=DEV):
        place = lax.rem(d + (p % DEV), DEV)
        return step(
            coef, x, below * flag(place >= by), above * flag(place + by <= DEV - 1)
        )

    def send_sums(block, j):
        block = block + pltpu.roll(block, 64, 1)
        block = block + pltpu.roll(block, 32, 1)
        block = block + pltpu.roll(block, 16, 1)
        row = jnp.sum(jnp.where(mine, block, 0.0), axis=0, keepdims=True)
        hz[j, pl.ds(15, 1)] = row
        srcz[j] = row
        for o in range(1, 16):
            send(srcz.at[j], hz.at[j, pl.ds(o - 1, 1)], rsend.at[j, 4], rrecv.at[j, 4], in_line(-o))

    def pass_sums(j):
        drain(hz.at[j, pl.ds(0, 15)], rrecv.at[j, 4])
        row = jnp.sum(hz[j], axis=0, keepdims=True)
        hp[j, pl.ds(15, 1)] = row
        srcp[j] = row
        for o in range(1, 16):
            send(srcp.at[j], hp.at[j, pl.ds(o - 1, 1)], rsend.at[j, 5], rrecv.at[j, 5], dev(-16 * o))

    def take_sums(j):
        drain(hp.at[j, pl.ds(0, 15)], rrecv.at[j, 5])
        total = jnp.sum(hp[j], axis=0, keepdims=True)
        return jnp.sum(jnp.where(mine, total, 0.0), axis=1, keepdims=True) * (1.0 / COUNT) + jnp.zeros((8, ROWS), F32)

    def finish(j, x, hess):
        sums = take_sums(j)
        h = [sums[i : i + 1] for i in range(3)]
        squares = sums[3:4]
        gr[lax.max(j - 1, 0)] = sums
        for i in range(3):
            squares = squares - 2.0 * (h[i] * h[i])
        for c in range(3):
            g = gr[c]
            for i in range(c + 1):
                squares = squares + (1.0 if i == c else 2.0) * (h[c] * h[i]) * g[4 + i : 5 + i]
        length = jnp.sqrt(jnp.maximum(squares, 0.0) + EPS)
        inverse = 1.0 / length
        new = x
        for i in range(3):
            new = new - h[i] * bs[i]
        new = new * inverse
        column = jnp.where(sub < 3, sums, 0.0)
        column = jnp.where(sub == j, length + jnp.zeros((8, ROWS), F32), column)
        hess = jnp.where(lane == j - 1, column, hess)
        return h, inverse, new, hess

    zero = jnp.zeros((8, ROWS), F32)
    for i in range(4):
        bs[i] = zero
    for i in range(3):
        gr[i] = zero
    for i in range(4):
        for c in range(3):
            xs[i, c] = zero

    r = rv[...]
    send_sums(jnp.where(sub == 3, jnp.sum(r * r, axis=0, keepdims=True) + zero, 0.0), 0)
    drain(h1.at[0], rrecv.at[0, 0])
    xs[0, 0] = h1[0, 0] * has_below
    xs[0, 1] = r
    xs[0, 2] = h1[0, 1] * has_above
    drain(near_c, mrecv.at[0])

    def body(j, hess):
        u = [xs[j, 0], xs[j, 1], xs[j, 2]]
        for level in range(NEAR):
            s = 2**level
            mid = step(cf.at[level], u[1], down(u[1], u[0], s), upward(u[1], u[2], s))
            if level < NEAR - 1:
                left = step(
                    near_c.at[0, level], u[0], down(u[0], u[0], s), upward(u[0], u[1], s)
                ) * has_below
                right = step(
                    near_c.at[1, level], u[2], down(u[2], u[1], s), upward(u[2], u[2], s)
                ) * has_above
                u = [left, mid, right]
            else:
                u = [None, mid, None]
        x = u[1]

        def group(x, src, got, slot, near_coef, level, by, later):
            src[j] = x
            for k, o in enumerate(LOWS):
                send(src.at[j], got.at[j, k], rsend.at[j, slot], rrecv.at[j, slot], dev(-o * by))
            pl.when(j == 0)(later)
            drain(got.at[j], rrecv.at[j, slot])
            f = {o: got[j, k] for k, o in enumerate(LOWS)}
            f[0] = x
            y = {
                0: far_level(cf.at[level], f[0], f[-1], f[1], 0, by),
                -2: far_level(near_coef.at[0], f[-2], f[-3], f[-1], -2 * by, by),
                2: far_level(near_coef.at[1], f[2], f[1], f[3], 2 * by, by),
            }
            return far_level(cf.at[level + 1], y[0], y[-2], y[2], 0, 2 * by)

        def after_first():
            send_low(False)
            send_top()
            drain(c7, mrecv.at[1])

        def after_second():
            send_operator()
            drain(c9, mrecv.at[2])

        x = group(x, src2, h2, 1, c7, 7, 1, after_first)
        x = group(x, src3, h3, 2, c9, 9, 4, after_second)

        srct[j] = x
        for o in range(1, 16):
            send(srct.at[j], ht.at[j, o - 1], rsend.at[j, 3], rrecv.at[j, 3], dev(-16 * o))
        pass_sums(j)

        @pl.when(j == 0)
        def _():
            drain(c11, mrecv.at[3])
            drain(c12, mrecv.at[4])
            drain(c13, mrecv.at[5])

        drain(ht.at[j], rrecv.at[j, 3])
        f = [x] + [ht[j, o] for o in range(15)]

        def top(coef, field, p, by):
            return far_level(
                coef, field[p], field[(p - by) % 16], field[(p + by) % 16], 16 * p, 16 * by
            )

        y1 = {p: top(cf.at[11] if p == 0 else c11.at[p // 2 - 1], f, p, 1) for p in range(0, 16, 2)}
        y2 = {p: top(cf.at[12] if p == 0 else c12.at[p // 4 - 1], y1, p, 2) for p in range(0, 16, 4)}
        y3 = {p: top(cf.at[13] if p == 0 else c13, y2, p, 4) for p in (0, 8)}
        x = top(cf.at[14], y3, 0, 8)
        x = x + mul(fv, x)

        src1[j] = x
        send(src1.at[j], h1.at[j + 1, 1], rsend.at[j + 1, 0], rrecv.at[j + 1, 0], dev(-1))
        send(src1.at[j], h1.at[j + 1, 0], rsend.at[j + 1, 0], rrecv.at[j + 1, 0], dev(1))

        h, inverse, new, hess = finish(j, xs[j, 1], hess)
        bs[j] = new
        basis_ref[j] = new

        @pl.when(j == 0)
        def _():
            drain(near_a, mrecv.at[6])

        drain(h1.at[j + 1], rrecv.at[j + 1, 0])
        cols = [h1[j + 1, 0] * has_below, x, h1[j + 1, 1] * has_above]
        for c, (coef, mask) in enumerate(
            ((near_a.at[0], has_below), (av, None), (near_a.at[1], has_above))
        ):
            v = 2.0 * cols[c] + mul(coef.at[0], cols[c])
            v = v + mul(coef.at[1], down(cols[c], cols[max(c - 1, 0)], 1))
            v = v + mul(coef.at[2], upward(cols[c], cols[min(c + 1, 2)], 1))
            for i in range(2):
                v = v - h[i] * xs[i + 1, c]
            v = v * inverse
            xs[j + 1, c] = v if mask is None else v * mask

        w = xs[j + 1, 1]
        sums = zero
        rows = [bs[0] * w, bs[1] * w, bs[2] * w, w * w, bs[0] * new, bs[1] * new, bs[2] * new]
        for i, row in enumerate(rows):
            sums = jnp.where(sub == i, jnp.sum(row, axis=0, keepdims=True) + zero, sums)
        send_sums(sums, j + 1)
        return hess

    hess = lax.fori_loop(0, ITERS, body, zero)
    pass_sums(ITERS)
    _, _, new, hess = finish(ITERS, xs[ITERS, 1], hess)
    basis_ref[ITERS] = new
    hess_ref[...] = hess

    drain(near_c, msend.at[0])
    drain(c7, msend.at[1])
    drain(c9, msend.at[2])
    drain(c11, msend.at[3])
    drain(c12, msend.at[4])
    drain(c13, msend.at[5])
    drain(near_a, msend.at[6])
    for j in range(ITERS + 1):
        drain(h1.at[j], rsend.at[j, 0])
        drain(hz.at[j, pl.ds(0, 15)], rsend.at[j, 4])
        drain(hp.at[j, pl.ds(0, 15)], rsend.at[j, 5])
        if j < ITERS:
            drain(h2.at[j], rsend.at[j, 1])
            drain(h3.at[j], rsend.at[j, 2])
            drain(ht.at[j], rsend.at[j, 3])


def hand_out(basis_ref, hess_ref, basis_out, hess_out):
    basis_out[...] = basis_ref[...]
    hess_out[...] = hess_ref[: ITERS + 1, :ITERS]


def on_device(right_side, diag_block, below_block, above_block, lower_level, upper_level, final_block):
    block = (64, ROWS)
    tile = (8, ROWS)
    vmem = lambda *lead: pltpu.VMEM(lead, F32)
    basis, hess = pl.pallas_call(
        kernel,
        out_shape=(
            jax.ShapeDtypeStruct((ITERS + 1, 8, ROWS), F32),
            jax.ShapeDtypeStruct(tile, F32),
        ),
        in_specs=[pl.BlockSpec(memory_space=pl.ANY)] * 7,
        out_specs=(pl.BlockSpec(memory_space=pltpu.VMEM), pl.BlockSpec(memory_space=pltpu.VMEM)),
        scratch_shapes=[
            vmem(*tile), vmem(3, *block), vmem(*block), vmem(15, 2, *block),
            vmem(2, 6, 2, *block), vmem(2, 3, *block), vmem(2, 2, *block), vmem(2, 2, *block),
            vmem(7, 2, *block), vmem(3, 2, *block), vmem(2, *block),
            vmem(4, 3, *tile), vmem(4, *tile), vmem(3, *tile),
            vmem(3, *tile), vmem(3, *tile), vmem(3, *tile), vmem(3, *tile),
            vmem(4, 1, ROWS), vmem(4, 1, ROWS),
            vmem(4, 2, *tile), vmem(3, 6, *tile), vmem(3, 6, *tile), vmem(3, 15, *tile),
            vmem(4, 16, ROWS), vmem(4, 16, ROWS),
            pltpu.SemaphoreType.DMA((7,)),
            pltpu.SemaphoreType.DMA((7,)),
            pltpu.SemaphoreType.DMA((7,)),
            pltpu.SemaphoreType.DMA((4, 6)),
            pltpu.SemaphoreType.DMA((4, 6)),
        ],
        compiler_params=pltpu.CompilerParams(collective_id=0, has_side_effects=True),
    )(
        right_side,
        diag_block.reshape(block),
        below_block.reshape(block),
        above_block.reshape(block),
        lower_level.reshape((15,) + block),
        upper_level.reshape((15,) + block),
        final_block.reshape(block),
    )
    return pl.pallas_call(
        hand_out,
        out_shape=(
            jax.ShapeDtypeStruct((ITERS + 1, 8, ROWS), F32),
            jax.ShapeDtypeStruct((ITERS + 1, ITERS), F32),
        ),
        in_specs=[pl.BlockSpec(memory_space=pltpu.VMEM)] * 2,
        out_specs=(pl.BlockSpec(memory_space=pltpu.VMEM), pl.BlockSpec(memory_space=pltpu.VMEM)),
    )(basis, hess)


def solution(mesh):
    blocks = P(None, None, "chain")
    levels = P(None, None, None, "chain")
    return jax.shard_map(
        on_device,
        mesh=mesh,
        in_specs=(P(None, "chain"), blocks, blocks, blocks, levels, levels, blocks),
        out_specs=(P(None, None, "chain"), P()),
        check_vma=False,
    )
```

```python
import functools

import jax
import jax.numpy as jnp
from jax import lax
from jax.experimental import pallas as pl
from jax.experimental.pallas import tpu as pltpu
from jax.sharding import PartitionSpec as P

ITERS = 3
EPS = 1e-06
DEV = 256
ROWS = 128
COUNT = 8 * DEV * ROWS
F32 = jnp.float32
NEAR = 7
LOWS = (-3, -2, -1, 1, 2, 3)


def kernel(
    r_hbm, dg_hbm, bl_hbm, ab_hbm, lo_hbm, up_hbm, fb_hbm,
    basis_ref, hess_ref,
    rv, av, fv, cf,
    near_c, near_a, c7, c9, c11, c12, c13,
    n_own, n11, n12, n13, n_fin,
    xs, bs, gr,
    src1, src2, src3, srct, srcz, srcp,
    h1, h2, h3, ht, hm, hz, hp,
    lsem, msend, mrecv, rsend, rrecv,
):
    d = lax.axis_index("chain")
    t = lax.rem(d, 16)
    line = d - t

    def dev(offset):
        return lax.rem(d + (offset % DEV), DEV)

    def in_line(offset):
        return line + lax.rem(t + (offset % 16), 16)

    loads = [
        pltpu.make_async_copy(r_hbm, rv, lsem.at[0]),
        pltpu.make_async_copy(lo_hbm, cf.at[:, 0], lsem.at[1]),
        pltpu.make_async_copy(up_hbm, cf.at[:, 1], lsem.at[2]),
        pltpu.make_async_copy(dg_hbm, av.at[0], lsem.at[3]),
        pltpu.make_async_copy(bl_hbm, av.at[1], lsem.at[4]),
        pltpu.make_async_copy(ab_hbm, av.at[2], lsem.at[5]),
        pltpu.make_async_copy(fb_hbm, fv, lsem.at[6]),
    ]
    for load in loads:
        load.start()

    partners = [dev(o) for o in (-12, -8, -4, -3, -2, -1, 1, 2, 3, 4, 8, 12)]
    partners += [dev(16 * o + c) for o in range(1, 16) for c in (-1, 0, 1)]
    partners += [in_line(o) for o in range(1, 16)]
    barrier = pltpu.get_barrier_semaphore()
    for other in partners:
        pl.semaphore_signal(barrier, inc=1, device_id=(other,), device_id_type=pl.DeviceIdType.MESH)
    pl.semaphore_wait(barrier, len(partners))

    def send(src, dst, ssem, rsem, other):
        pltpu.make_async_remote_copy(
            src_ref=src, dst_ref=dst, send_sem=ssem, recv_sem=rsem,
            device_id=(other,), device_id_type=pl.DeviceIdType.MESH,
        ).start()

    def drain(buf, sem):
        pltpu.make_async_copy(buf, buf, sem).wait()

    for load in loads:
        load.wait()

    def pass_ends(j, src):
        send(src, h1.at[j, 1], rsend.at[j, 0], rrecv.at[j, 0], dev(-1))
        send(src, h1.at[j, 0], rsend.at[j, 0], rrecv.at[j, 0], dev(1))

    pass_ends(0, rv)
    send(cf.at[pl.ds(0, 6)], near_c.at[1], msend.at[0], mrecv.at[0], dev(-1))
    send(cf.at[pl.ds(0, 6)], near_c.at[0], msend.at[0], mrecv.at[0], dev(1))

    def send_low(first):
        if first:
            send(cf.at[7], c7.at[1], msend.at[1], mrecv.at[1], dev(-2))
            send(cf.at[7], c7.at[0], msend.at[1], mrecv.at[1], dev(2))
        else:
            send(cf.at[9], c9.at[1], msend.at[2], mrecv.at[2], dev(-8))
            send(cf.at[9], c9.at[0], msend.at[2], mrecv.at[2], dev(8))

    def send_top():
        for p in range(2, 16, 2):
            send(cf.at[11], c11.at[p // 2 - 1], msend.at[3], mrecv.at[3], dev(-16 * p))
        for p in range(4, 16, 4):
            send(cf.at[12], c12.at[p // 4 - 1], msend.at[4], mrecv.at[4], dev(-16 * p))
        send(cf.at[13], c13, msend.at[5], mrecv.at[5], dev(-16 * 8))

    def pass_on(k, src, dst):
        send(src, dst.at[1], msend.at[k], mrecv.at[k], dev(-1))
        send(src, dst.at[0], msend.at[k], mrecv.at[k], dev(1))

    def send_operator():
        send(av, near_a.at[1], msend.at[6], mrecv.at[6], dev(-1))
        send(av, near_a.at[0], msend.at[6], mrecv.at[6], dev(1))

    send_low(True)

    lane = lax.broadcasted_iota(jnp.int32, (8, ROWS), 1)
    sub = lax.broadcasted_iota(jnp.int32, (8, ROWS), 0)
    mine = (lane >= 16 * sub) & (lane < 16 * sub + 16)

    def flag(cond):
        return jnp.where(cond, 1.0, 0.0).astype(F32)

    has_below, has_above = flag(d >= 1), flag(d <= DEV - 2)

    def mul(blocks, v):
        total = blocks[pl.ds(0, 8, stride=8), :] * v[0:1]
        for b in range(1, 8):
            total = total + blocks[pl.ds(b, 8, stride=8), :] * v[b : b + 1]
        return total

    def step(coef, x, below, above):
        return x + mul(coef.at[0], below) + mul(coef.at[1], above)

    def down(u, prev, s):
        return jnp.where(lane < s, pltpu.roll(prev, s, 1), pltpu.roll(u, s, 1))

    def upward(u, following, s):
        return jnp.where(
            lane >= ROWS - s, pltpu.roll(following, ROWS - s, 1), pltpu.roll(u, ROWS - s, 1)
        )

    def far_level(coef, x, below, above, p, by, scale=1, size=DEV):
        place = lax.rem(d + (p % DEV), DEV)
        return step(
            coef, x, below * flag(place >= by), above * flag(place + by <= DEV - 1)
        )

    def send_sums(block, j):
        block = block + pltpu.roll(block, 64, 1)
        block = block + pltpu.roll(block, 32, 1)
        block = block + pltpu.roll(block, 16, 1)
        row = jnp.sum(jnp.where(mine, block, 0.0), axis=0, keepdims=True)
        hz[j, pl.ds(15, 1)] = row
        srcz[j] = row
        for o in range(1, 16):
            send(srcz.at[j], hz.at[j, pl.ds(o - 1, 1)], rsend.at[j, 4], rrecv.at[j, 4], in_line(-o))

    def pass_sums(j):
        drain(hz.at[j, pl.ds(0, 15)], rrecv.at[j, 4])
        row = jnp.sum(hz[j], axis=0, keepdims=True)
        hp[j, pl.ds(15, 1)] = row
        srcp[j] = row
        for o in range(1, 16):
            send(srcp.at[j], hp.at[j, pl.ds(o - 1, 1)], rsend.at[j, 5], rrecv.at[j, 5], dev(-16 * o))

    def take_sums(j):
        drain(hp.at[j, pl.ds(0, 15)], rrecv.at[j, 5])
        total = jnp.sum(hp[j], axis=0, keepdims=True)
        return jnp.sum(jnp.where(mine, total, 0.0), axis=1, keepdims=True) * (1.0 / COUNT) + jnp.zeros((8, ROWS), F32)

    def finish(j, x, hess):
        sums = take_sums(j)
        h = [sums[i : i + 1] for i in range(3)]
        squares = sums[3:4]
        gr[lax.max(j - 1, 0)] = sums
        for i in range(3):
            squares = squares - 2.0 * (h[i] * h[i])
        for c in range(3):
            g = gr[c]
            for i in range(c + 1):
                squares = squares + (1.0 if i == c else 2.0) * (h[c] * h[i]) * g[4 + i : 5 + i]
        length = jnp.sqrt(jnp.maximum(squares, 0.0) + EPS)
        inverse = 1.0 / length
        new = x
        for i in range(3):
            new = new - h[i] * bs[i]
        new = new * inverse
        column = jnp.where(sub < 3, sums, 0.0)
        column = jnp.where(sub == j, length + jnp.zeros((8, ROWS), F32), column)
        hess = jnp.where(lane == j - 1, column, hess)
        return h, inverse, new, hess

    zero = jnp.zeros((8, ROWS), F32)
    for i in range(4):
        bs[i] = zero
    for i in range(3):
        gr[i] = zero
    for i in range(4):
        for c in range(3):
            xs[i, c] = zero

    r = rv[...]
    send_sums(jnp.where(sub == 3, jnp.sum(r * r, axis=0, keepdims=True) + zero, 0.0), 0)
    drain(h1.at[0], rrecv.at[0, 0])
    xs[0, 0] = h1[0, 0] * has_below
    xs[0, 1] = r
    xs[0, 2] = h1[0, 1] * has_above
    drain(near_c, mrecv.at[0])

    def body(j, hess, first=False):
        u = [xs[j, 0], xs[j, 1], xs[j, 2]]
        for level in range(NEAR):
            s = 2**level
            mid = step(cf.at[level], u[1], down(u[1], u[0], s), upward(u[1], u[2], s))
            if level < NEAR - 1:
                left = step(
                    near_c.at[0, level], u[0], down(u[0], u[0], s), upward(u[0], u[1], s)
                ) * has_below
                right = step(
                    near_c.at[1, level], u[2], down(u[2], u[1], s), upward(u[2], u[2], s)
                ) * has_above
                u = [left, mid, right]
            else:
                u = [None, mid, None]
        x = u[1]

        def group(x, src, got, slot, near_coef, level, by, later):
            src[j] = x
            for k, o in enumerate(LOWS):
                send(src.at[j], got.at[j, k], rsend.at[j, slot], rrecv.at[j, slot], dev(-o * by))
            later()
            drain(got.at[j], rrecv.at[j, slot])
            f = {o: got[j, k] for k, o in enumerate(LOWS)}
            f[0] = x
            y = {
                0: far_level(cf.at[level], f[0], f[-1], f[1], 0, by),
                -2: far_level(near_coef.at[0], f[-2], f[-3], f[-1], -2 * by, by),
                2: far_level(near_coef.at[1], f[2], f[1], f[3], 2 * by, by),
            }
            return far_level(cf.at[level + 1], y[0], y[-2], y[2], 0, 2 * by)

        def after_first():
            if first:
                send_low(False)
                send_top()
                drain(c7, mrecv.at[1])
            else:
                pl.when(j == 1)(lambda: pass_on(8, cf.at[pl.ds(11, 4)], n_own))

        def after_second():
            if first:
                send_operator()
                drain(c9, mrecv.at[2])
            else:

                @pl.when(j == 1)
                def _():
                    pass_on(9, c12, n12)
                    pass_on(10, c13, n13)
                    pass_on(11, fv, n_fin)

        x = group(x, src2, h2, 1, c7, 7, 1, after_first)
        x = group(x, src3, h3, 2, c9, 9, 4, after_second)

        srct[j] = x
        slots = [(0, o) for o in range(1, 16)]
        if not first:
            slots += [(c, o) for c in (-1, 1) for o in range(16)]
        got = ht if first else hm.at[j - 1]
        for k, (c, o) in enumerate(slots):
            send(srct.at[j], got.at[k], rsend.at[j, 3], rrecv.at[j, 3], dev(-16 * o - c))
        pass_sums(j)

        if first:
            drain(c11, mrecv.at[3])
            drain(c12, mrecv.at[4])
            drain(c13, mrecv.at[5])
        else:

            @pl.when(j == 1)
            def _():
                drain(n11, mrecv.at[7])
                drain(n_own, mrecv.at[8])
                drain(n12, mrecv.at[9])
                drain(n13, mrecv.at[10])
                drain(n_fin, mrecv.at[11])

        drain(got, rrecv.at[j, 3])
        fields = {(0, 0): x}
        for k, key in enumerate(slots):
            fields[key] = got[k]

        def column(c):
            if c == 0:
                own, others, final = cf.at[pl.ds(11, 4)], (c11, c12, c13), fv
            else:
                side = max(c, 0)
                own = n_own.at[side]
                others, final = (n11.at[side], n12.at[side], n13.at[side]), n_fin.at[side]
            y = [fields[c, o] for o in range(16)]
            for rank in range(4):
                by = 2**rank

                def coef(p):
                    if p == 0:
                        return own.at[rank]
                    return others[2] if rank == 2 else others[rank].at[p // (2 * by) - 1]

                places = range(0, 16, 2 * by)
                y = {
                    p: far_level(
                        coef(p), y[p], y[(p - by) % 16], y[(p + by) % 16], 16 * p + c, 16 * by
                    )
                    for p in places
                }
            return y[0] + mul(final, y[0])

        x = column(0)
        if first:
            src1[...] = x
            pass_ends(1, src1)
            pass_on(7, c11, n11)
        else:
            sides = column(-1), column(1)

        h, inverse, new, hess = finish(j, xs[j, 1], hess)
        bs[j] = new
        basis_ref[j] = new

        if first:
            drain(near_a, mrecv.at[6])
            drain(h1.at[1], rrecv.at[1, 0])
            sides = h1[1, 0], h1[1, 1]
        cols = [sides[0] * has_below, x, sides[1] * has_above]
        for c, (coef, mask) in enumerate(
            ((near_a.at[0], has_below), (av, None), (near_a.at[1], has_above))
        ):
            v = 2.0 * cols[c] + mul(coef.at[0], cols[c])
            v = v + mul(coef.at[1], down(cols[c], cols[max(c - 1, 0)], 1))
            v = v + mul(coef.at[2], upward(cols[c], cols[min(c + 1, 2)], 1))
            for i in range(2):
                v = v - h[i] * xs[i + 1, c]
            v = v * inverse
            xs[j + 1, c] = v if mask is None else v * mask

        w = xs[j + 1, 1]
        sums = zero
        rows = [bs[0] * w, bs[1] * w, bs[2] * w, w * w, bs[0] * new, bs[1] * new, bs[2] * new]
        for i, row in enumerate(rows):
            sums = jnp.where(sub == i, jnp.sum(row, axis=0, keepdims=True) + zero, sums)
        send_sums(sums, j + 1)
        return hess

    hess = body(0, zero, True)
    hess = lax.fori_loop(1, ITERS, body, hess)
    pass_sums(ITERS)
    _, _, new, hess = finish(ITERS, xs[ITERS, 1], hess)
    basis_ref[ITERS] = new
    hess_ref[...] = hess

    drain(near_c, msend.at[0])
    drain(c7, msend.at[1])
    drain(c9, msend.at[2])
    drain(c11, msend.at[3])
    drain(c12, msend.at[4])
    drain(c13, msend.at[5])
    drain(near_a, msend.at[6])
    for k, buf in enumerate((n11, n_own, n12, n13, n_fin)):
        drain(buf, msend.at[7 + k])
    for j in range(ITERS + 1):
        drain(hz.at[j, pl.ds(0, 15)], rsend.at[j, 4])
        drain(hp.at[j, pl.ds(0, 15)], rsend.at[j, 5])
        if j < 2:
            drain(h1.at[j], rsend.at[j, 0])
        if j < ITERS:
            drain(h2.at[j], rsend.at[j, 1])
            drain(h3.at[j], rsend.at[j, 2])
            drain(ht if j == 0 else hm.at[j - 1], rsend.at[j, 3])


def hand_out(basis_ref, hess_ref, basis_out, hess_out):
    basis_out[...] = basis_ref[...]
    hess_out[...] = hess_ref[: ITERS + 1, :ITERS]


def on_device(right_side, diag_block, below_block, above_block, lower_level, upper_level, final_block):
    block = (64, ROWS)
    tile = (8, ROWS)
    vmem = lambda *lead: pltpu.VMEM(lead, F32)
    basis, hess = pl.pallas_call(
        kernel,
        out_shape=(
            jax.ShapeDtypeStruct((ITERS + 1, 8, ROWS), F32),
            jax.ShapeDtypeStruct(tile, F32),
        ),
        in_specs=[pl.BlockSpec(memory_space=pl.ANY)] * 7,
        out_specs=(pl.BlockSpec(memory_space=pltpu.VMEM), pl.BlockSpec(memory_space=pltpu.VMEM)),
        scratch_shapes=[
            vmem(*tile), vmem(3, *block), vmem(*block), vmem(15, 2, *block),
            vmem(2, 6, 2, *block), vmem(2, 3, *block), vmem(2, 2, *block), vmem(2, 2, *block),
            vmem(7, 2, *block), vmem(3, 2, *block), vmem(2, *block),
            vmem(2, 4, 2, *block), vmem(2, 7, 2, *block), vmem(2, 3, 2, *block), vmem(2, 2, *block),
            vmem(2, *block),
            vmem(4, 3, *tile), vmem(4, *tile), vmem(3, *tile),
            vmem(*tile), vmem(3, *tile), vmem(3, *tile), vmem(3, *tile),
            vmem(4, 1, ROWS), vmem(4, 1, ROWS),
            vmem(2, 2, *tile), vmem(3, 6, *tile), vmem(3, 6, *tile), vmem(15, *tile), vmem(2, 47, *tile),
            vmem(4, 16, ROWS), vmem(4, 16, ROWS),
            pltpu.SemaphoreType.DMA((7,)),
            pltpu.SemaphoreType.DMA((12,)),
            pltpu.SemaphoreType.DMA((12,)),
            pltpu.SemaphoreType.DMA((4, 6)),
            pltpu.SemaphoreType.DMA((4, 6)),
        ],
        compiler_params=pltpu.CompilerParams(collective_id=0, has_side_effects=True),
    )(
        right_side,
        diag_block.reshape(block),
        below_block.reshape(block),
        above_block.reshape(block),
        lower_level.reshape((15,) + block),
        upper_level.reshape((15,) + block),
        final_block.reshape(block),
    )
    return pl.pallas_call(
        hand_out,
        out_shape=(
            jax.ShapeDtypeStruct((ITERS + 1, 8, ROWS), F32),
            jax.ShapeDtypeStruct((ITERS + 1, ITERS), F32),
        ),
        in_specs=[pl.BlockSpec(memory_space=pltpu.VMEM)] * 2,
        out_specs=(pl.BlockSpec(memory_space=pltpu.VMEM), pl.BlockSpec(memory_space=pltpu.VMEM)),
    )(basis, hess)


def solution(mesh):
    blocks = P(None, None, "chain")
    levels = P(None, None, None, "chain")
    return jax.shard_map(
        on_device,
        mesh=mesh,
        in_specs=(P(None, "chain"), blocks, blocks, blocks, levels, levels, blocks),
        out_specs=(P(None, None, "chain"), P()),
        check_vma=False,
    )
```

```python
import functools

import jax
import jax.numpy as jnp
from jax import lax
from jax.experimental import pallas as pl
from jax.experimental.pallas import tpu as pltpu
from jax.sharding import PartitionSpec as P

ITERS = 3
EPS = 1e-06
DEV = 256
ROWS = 128
COUNT = 8 * DEV * ROWS
F32 = jnp.float32
NEAR = 7
LOWS = (-3, -2, -1, 1, 2, 3)


def kernel(
    r_hbm, dg_hbm, bl_hbm, ab_hbm, lo_hbm, up_hbm, fb_hbm,
    basis_ref, hess_ref,
    rv, av, fv, cf,
    packs, got_packs, near_c, near_a, c7, c9, c11, c12, c13,
    xs, bs, gr,
    src1, src2, src3, srct, srcz, srcp,
    h1, h2, h3, ht, hz, hp,
    lsem, msend, mrecv, rsend, rrecv,
):
    d = lax.axis_index("chain")
    t = lax.rem(d, 16)
    line = d - t

    def dev(offset):
        return lax.rem(d + (offset % DEV), DEV)

    def in_line(offset):
        return line + lax.rem(t + (offset % 16), 16)

    loads = [
        pltpu.make_async_copy(r_hbm, rv, lsem.at[0]),
        pltpu.make_async_copy(lo_hbm, cf.at[:, 0], lsem.at[1]),
        pltpu.make_async_copy(up_hbm, cf.at[:, 1], lsem.at[2]),
        pltpu.make_async_copy(dg_hbm, av.at[0], lsem.at[3]),
        pltpu.make_async_copy(bl_hbm, av.at[1], lsem.at[4]),
        pltpu.make_async_copy(ab_hbm, av.at[2], lsem.at[5]),
        pltpu.make_async_copy(fb_hbm, fv, lsem.at[6]),
    ]
    for load in loads:
        load.start()

    partners = [dev(o) for o in (-12, -8, -4, -3, -2, -1, 1, 2, 3, 4, 8, 12)]
    partners += [dev(16 * o) for o in range(1, 16)]
    partners += [in_line(o) for o in range(1, 16)]
    barrier = pltpu.get_barrier_semaphore()
    for other in partners:
        pl.semaphore_signal(barrier, inc=1, device_id=(other,), device_id_type=pl.DeviceIdType.MESH)

    def send(src, dst, ssem, rsem, other):
        pltpu.make_async_remote_copy(
            src_ref=src, dst_ref=dst, send_sem=ssem, recv_sem=rsem,
            device_id=(other,), device_id_type=pl.DeviceIdType.MESH,
        ).start()

    def drain(buf, sem):
        pltpu.make_async_copy(buf, buf, sem).wait()

    for load in loads:
        load.wait()

    def send_low(first):
        if first:
            send(cf.at[7], c7.at[1], msend.at[1], mrecv.at[1], dev(-2))
            send(cf.at[7], c7.at[0], msend.at[1], mrecv.at[1], dev(2))
        else:
            send(cf.at[9], c9.at[1], msend.at[2], mrecv.at[2], dev(-8))
            send(cf.at[9], c9.at[0], msend.at[2], mrecv.at[2], dev(8))

    def send_top():
        for p in range(2, 16, 2):
            send(cf.at[11], c11.at[p // 2 - 1], msend.at[3], mrecv.at[3], dev(-16 * p))
        for p in range(4, 16, 4):
            send(cf.at[12], c12.at[p // 4 - 1], msend.at[4], mrecv.at[4], dev(-16 * p))
        send(cf.at[13], c13, msend.at[5], mrecv.at[5], dev(-16 * 8))

    lane = lax.broadcasted_iota(jnp.int32, (8, ROWS), 1)
    sub = lax.broadcasted_iota(jnp.int32, (8, ROWS), 0)
    mine = (lane >= 16 * sub) & (lane < 16 * sub + 16)

    def flag(cond):
        return jnp.where(cond, 1.0, 0.0).astype(F32)

    has_below, has_above = flag(d >= 1), flag(d <= DEV - 2)

    def mul(blocks, v):
        total = blocks[pl.ds(0, 8, stride=8), :] * v[0:1]
        for b in range(1, 8):
            total = total + blocks[pl.ds(b, 8, stride=8), :] * v[b : b + 1]
        return total

    def step(coef, x, below, above):
        return x + mul(coef.at[0], below) + mul(coef.at[1], above)

    def down(u, prev, s):
        return jnp.where(lane < s, pltpu.roll(prev, s, 1), pltpu.roll(u, s, 1))

    def upward(u, following, s):
        return jnp.where(
            lane >= ROWS - s, pltpu.roll(following, ROWS - s, 1), pltpu.roll(u, ROWS - s, 1)
        )

    def far_level(coef, x, below, above, p, by, scale=1, size=DEV):
        place = lax.rem(d + (p % DEV), DEV)
        return step(
            coef, x, below * flag(place >= by), above * flag(place + by <= DEV - 1)
        )

    def send_sums(block, j):
        block = block + pltpu.roll(block, 64, 1)
        block = block + pltpu.roll(block, 32, 1)
        block = block + pltpu.roll(block, 16, 1)
        row = jnp.sum(jnp.where(mine, block, 0.0), axis=0, keepdims=True)
        hz[j, pl.ds(15, 1)] = row
        srcz[j] = row
        for o in range(1, 16):
            send(srcz.at[j], hz.at[j, pl.ds(o - 1, 1)], rsend.at[j, 4], rrecv.at[j, 4], in_line(-o))

    def pass_sums(j):
        drain(hz.at[j, pl.ds(0, 15)], rrecv.at[j, 4])
        row = jnp.sum(hz[j], axis=0, keepdims=True)
        hp[j, pl.ds(15, 1)] = row
        srcp[j] = row
        for o in range(1, 16):
            send(srcp.at[j], hp.at[j, pl.ds(o - 1, 1)], rsend.at[j, 5], rrecv.at[j, 5], dev(-16 * o))

    def take_sums(j):
        drain(hp.at[j, pl.ds(0, 15)], rrecv.at[j, 5])
        total = jnp.sum(hp[j], axis=0, keepdims=True)
        return jnp.sum(jnp.where(mine, total, 0.0), axis=1, keepdims=True) * (1.0 / COUNT) + jnp.zeros((8, ROWS), F32)

    def finish(j, x, hess):
        sums = take_sums(j)
        h = [sums[i : i + 1] for i in range(3)]
        squares = sums[3:4]
        gr[lax.max(j - 1, 0)] = sums
        for i in range(3):
            squares = squares - 2.0 * (h[i] * h[i])
        for c in range(3):
            g = gr[c]
            for i in range(c + 1):
                squares = squares + (1.0 if i == c else 2.0) * (h[c] * h[i]) * g[4 + i : 5 + i]
        length = jnp.sqrt(jnp.maximum(squares, 0.0) + EPS)
        inverse = 1.0 / length
        new = x
        for i in range(3):
            new = new - h[i] * bs[i]
        new = new * inverse
        column = jnp.where(sub < 3, sums, 0.0)
        column = jnp.where(sub == j, length + jnp.zeros((8, ROWS), F32), column)
        hess = jnp.where(lane == j - 1, column, hess)
        return h, inverse, new, hess

    def make_strips(j, f, w):
        low, high, v = f, f, w
        for level in range(NEAR - 1):
            s = 2**level
            low = jnp.where(lane >= 2 * s, pltpu.roll(v, s, 1), low)
            high = jnp.where(lane < ROWS - 2 * s, pltpu.roll(v, ROWS - s, 1), high)
            if level < NEAR - 2:
                v = step(cf.at[level], v, pltpu.roll(v, s, 1), pltpu.roll(v, ROWS - s, 1))
        src1[j, 0] = low
        src1[j, 1] = high

    def ship_strips(j):
        send(src1.at[j, 0], h1.at[j, 1], rsend.at[j, 0], rrecv.at[j, 0], dev(-1))
        send(src1.at[j, 1], h1.at[j, 0], rsend.at[j, 0], rrecv.at[j, 0], dev(1))

    zero = jnp.zeros((8, ROWS), F32)
    for i in range(4):
        bs[i] = zero
    for i in range(3):
        gr[i] = zero
    for i in range(4):
        for c in range(3):
            xs[i, c] = zero

    r = rv[...]
    make_strips(0, r, r)
    wide = lax.broadcasted_iota(jnp.int32, (64, ROWS), 1)

    for which in range(2):
        low = jnp.where(wide < 1, av[1 + which], pltpu.roll(av[0], 1, 1))
        high = jnp.where(wide >= ROWS - 1, av[1 + which], pltpu.roll(av[0], ROWS - 1, 1))
        for level in range(NEAR - 1):
            w = 2 ** (level + 1)
            low = jnp.where(wide >= w, pltpu.roll(cf[level, which], w, 1), low)
            high = jnp.where(wide < ROWS - w, pltpu.roll(cf[level, which], ROWS - w, 1), high)
        packs[0, which] = low
        packs[1, which] = high
    pl.semaphore_wait(barrier, len(partners))
    ship_strips(0)
    send(packs.at[0], got_packs.at[1], msend.at[0], mrecv.at[0], dev(-1))
    send(packs.at[1], got_packs.at[0], msend.at[0], mrecv.at[0], dev(1))
    send_low(True)
    send_sums(jnp.where(sub == 3, jnp.sum(r * r, axis=0, keepdims=True) + zero, 0.0), 0)
    drain(h1.at[0], rrecv.at[0, 0])
    xs[0, 0] = h1[0, 0] * has_below
    xs[0, 1] = r
    xs[0, 2] = h1[0, 1] * has_above
    drain(got_packs, mrecv.at[0])
    for side in range(2):
        for which in range(2):
            pack = got_packs[side, which]
            near_a[side, 1 + which] = pack
            for level in range(NEAR - 1):
                w = 2 ** (level + 1)
                near_c[side, level, which] = pltpu.roll(pack, w if side == 0 else ROWS - w, 1)
        near_a[side, 0] = pltpu.roll(got_packs[side, 0], 1 if side == 0 else ROWS - 1, 1)

    def body(j, hess):
        strip = [h1[j, 0] * has_below, h1[j, 1] * has_above]

        def join(left, right, k):
            return (
                jnp.where(lane >= ROWS - k, left, pltpu.roll(strip[0], k, 1)),
                jnp.where(lane < k, right, pltpu.roll(strip[1], ROWS - k, 1)),
            )

        left, right = join(xs[j, 0], xs[j, 2], 1)
        u = [left, xs[j, 1], right]
        for level in range(NEAR):
            s = 2**level
            mid = step(cf.at[level], u[1], down(u[1], u[0], s), upward(u[1], u[2], s))
            if level < NEAR - 1:
                left = step(
                    near_c.at[0, level], u[0], down(u[0], u[0], s), upward(u[0], u[1], s)
                ) * has_below
                right = step(
                    near_c.at[1, level], u[2], down(u[2], u[1], s), upward(u[2], u[2], s)
                ) * has_above
                if level < NEAR - 2:
                    left, right = join(left, right, 2 * s)
                u = [left, mid, right]
            else:
                u = [None, mid, None]
        x = u[1]

        def group(x, src, got, slot, near_coef, level, by, later):
            src[j] = x
            for k, o in enumerate(LOWS):
                send(src.at[j], got.at[j, k], rsend.at[j, slot], rrecv.at[j, slot], dev(-o * by))
            pl.when(j == 0)(later)
            drain(got.at[j], rrecv.at[j, slot])
            f = {o: got[j, k] for k, o in enumerate(LOWS)}
            f[0] = x
            y = {
                0: far_level(cf.at[level], f[0], f[-1], f[1], 0, by),
                -2: far_level(near_coef.at[0], f[-2], f[-3], f[-1], -2 * by, by),
                2: far_level(near_coef.at[1], f[2], f[1], f[3], 2 * by, by),
            }
            return far_level(cf.at[level + 1], y[0], y[-2], y[2], 0, 2 * by)

        def after_first():
            send_low(False)
            send_top()
            drain(c7, mrecv.at[1])

        def after_second():
            drain(c9, mrecv.at[2])

        x = group(x, src2, h2, 1, c7, 7, 1, after_first)
        x = group(x, src3, h3, 2, c9, 9, 4, after_second)

        srct[j] = x
        for o in range(1, 16):
            send(srct.at[j], ht.at[j, o - 1], rsend.at[j, 3], rrecv.at[j, 3], dev(-16 * o))
        pass_sums(j)

        @pl.when(j == 0)
        def _():
            drain(c11, mrecv.at[3])
            drain(c12, mrecv.at[4])
            drain(c13, mrecv.at[5])

        drain(ht.at[j], rrecv.at[j, 3])
        f = [x] + [ht[j, o] for o in range(15)]

        def top(coef, field, p, by):
            return far_level(
                coef, field[p], field[(p - by) % 16], field[(p + by) % 16], 16 * p, 16 * by
            )

        y1 = {p: top(cf.at[11] if p == 0 else c11.at[p // 2 - 1], f, p, 1) for p in range(0, 16, 2)}
        y2 = {p: top(cf.at[12] if p == 0 else c12.at[p // 4 - 1], y1, p, 2) for p in range(0, 16, 4)}
        y3 = {p: top(cf.at[13] if p == 0 else c13, y2, p, 4) for p in (0, 8)}
        x = top(cf.at[14], y3, 0, 8)
        x = x + mul(fv, x)

        h, inverse, new, hess = finish(j, xs[j, 1], hess)
        bs[j] = new
        basis_ref[j] = new

        def operate(coef, c, f, below, above):
            v = 2.0 * f + mul(coef.at[0], f) + mul(coef.at[1], below) + mul(coef.at[2], above)
            for i in range(2):
                v = v - h[i] * xs[i + 1, c]
            return v * inverse

        make_strips(j + 1, x, operate(av, 1, x, pltpu.roll(x, 1, 1), pltpu.roll(x, ROWS - 1, 1)))
        ship_strips(j + 1)
        drain(h1.at[j + 1], rrecv.at[j + 1, 0])
        left, right = h1[j + 1, 0] * has_below, h1[j + 1, 1] * has_above
        middle = operate(av, 1, x, down(x, left, 1), upward(x, right, 1))
        left = operate(near_a.at[0], 0, left, down(left, left, 1), upward(left, x, 1))
        right = operate(near_a.at[1], 2, right, down(right, x, 1), upward(right, right, 1))
        xs[j + 1, 0] = left * has_below
        xs[j + 1, 1] = middle
        xs[j + 1, 2] = right * has_above

        w = xs[j + 1, 1]
        sums = zero
        rows = [bs[0] * w, bs[1] * w, bs[2] * w, w * w, bs[0] * new, bs[1] * new, bs[2] * new]
        for i, row in enumerate(rows):
            sums = jnp.where(sub == i, jnp.sum(row, axis=0, keepdims=True) + zero, sums)
        send_sums(sums, j + 1)
        return hess

    hess = lax.fori_loop(0, ITERS, body, zero)
    pass_sums(ITERS)
    _, _, new, hess = finish(ITERS, xs[ITERS, 1], hess)
    basis_ref[ITERS] = new
    hess_ref[...] = hess

    drain(packs, msend.at[0])
    drain(c7, msend.at[1])
    drain(c9, msend.at[2])
    drain(c11, msend.at[3])
    drain(c12, msend.at[4])
    drain(c13, msend.at[5])
    for j in range(ITERS + 1):
        drain(h1.at[j], rsend.at[j, 0])
        drain(hz.at[j, pl.ds(0, 15)], rsend.at[j, 4])
        drain(hp.at[j, pl.ds(0, 15)], rsend.at[j, 5])
        if j < ITERS:
            drain(h2.at[j], rsend.at[j, 1])
            drain(h3.at[j], rsend.at[j, 2])
            drain(ht.at[j], rsend.at[j, 3])


def hand_out(basis_ref, hess_ref, basis_out, hess_out):
    basis_out[...] = basis_ref[...]
    hess_out[...] = hess_ref[: ITERS + 1, :ITERS]


def on_device(right_side, diag_block, below_block, above_block, lower_level, upper_level, final_block):
    block = (64, ROWS)
    tile = (8, ROWS)
    vmem = lambda *lead: pltpu.VMEM(lead, F32)
    basis, hess = pl.pallas_call(
        kernel,
        out_shape=(
            jax.ShapeDtypeStruct((ITERS + 1, 8, ROWS), F32),
            jax.ShapeDtypeStruct(tile, F32),
        ),
        in_specs=[pl.BlockSpec(memory_space=pl.ANY)] * 7,
        out_specs=(pl.BlockSpec(memory_space=pltpu.VMEM), pl.BlockSpec(memory_space=pltpu.VMEM)),
        scratch_shapes=[
            vmem(*tile), vmem(3, *block), vmem(*block), vmem(15, 2, *block),
            vmem(2, 2, *block), vmem(2, 2, *block), vmem(2, 6, 2, *block), vmem(2, 3, *block), vmem(2, 2, *block), vmem(2, 2, *block),
            vmem(7, 2, *block), vmem(3, 2, *block), vmem(2, *block),
            vmem(4, 3, *tile), vmem(4, *tile), vmem(3, *tile),
            vmem(4, 2, *tile), vmem(3, *tile), vmem(3, *tile), vmem(3, *tile),
            vmem(4, 1, ROWS), vmem(4, 1, ROWS),
            vmem(4, 2, *tile), vmem(3, 6, *tile), vmem(3, 6, *tile), vmem(3, 15, *tile),
            vmem(4, 16, ROWS), vmem(4, 16, ROWS),
            pltpu.SemaphoreType.DMA((7,)),
            pltpu.SemaphoreType.DMA((7,)),
            pltpu.SemaphoreType.DMA((7,)),
            pltpu.SemaphoreType.DMA((4, 6)),
            pltpu.SemaphoreType.DMA((4, 6)),
        ],
        compiler_params=pltpu.CompilerParams(collective_id=0, has_side_effects=True),
    )(
        right_side,
        diag_block.reshape(block),
        below_block.reshape(block),
        above_block.reshape(block),
        lower_level.reshape((15,) + block),
        upper_level.reshape((15,) + block),
        final_block.reshape(block),
    )
    return pl.pallas_call(
        hand_out,
        out_shape=(
            jax.ShapeDtypeStruct((ITERS + 1, 8, ROWS), F32),
            jax.ShapeDtypeStruct((ITERS + 1, ITERS), F32),
        ),
        in_specs=[pl.BlockSpec(memory_space=pltpu.VMEM)] * 2,
        out_specs=(pl.BlockSpec(memory_space=pltpu.VMEM), pl.BlockSpec(memory_space=pltpu.VMEM)),
    )(basis, hess)


def solution(mesh):
    blocks = P(None, None, "chain")
    levels = P(None, None, None, "chain")
    return jax.shard_map(
        on_device,
        mesh=mesh,
        in_specs=(P(None, "chain"), blocks, blocks, blocks, levels, levels, blocks),
        out_specs=(P(None, None, "chain"), P()),
        check_vma=False,
    )
```

```python
import functools

import jax
import jax.numpy as jnp
from jax import lax
from jax.experimental import pallas as pl
from jax.experimental.pallas import tpu as pltpu
from jax.sharding import PartitionSpec as P

ITERS = 3
EPS = 1e-06
DEV = 256
ROWS = 128
COUNT = 8 * DEV * ROWS
F32 = jnp.float32
NEAR = 7
LOWS = (-3, -2, -1, 1, 2, 3)


def kernel(
    r_hbm, dg_hbm, bl_hbm, ab_hbm, lo_hbm, up_hbm, fb_hbm,
    basis_ref, hess_ref,
    rv, av, fv, cf,
    packs, got_packs, near_c, near_a, c7, c9, c11, c12, c13,
    edges, got_edges, edge_c, edge_f,
    xs, bs, gr,
    src1, src2, src3, srct, srcz, srcp,
    h1, h2, h3, ht, hm, hz, hp,
    lsem, msend, mrecv, rsend, rrecv,
):
    d = lax.axis_index("chain")
    t = lax.rem(d, 16)
    line = d - t

    def dev(offset):
        return lax.rem(d + (offset % DEV), DEV)

    def in_line(offset):
        return line + lax.rem(t + (offset % 16), 16)

    loads = [
        pltpu.make_async_copy(r_hbm, rv, lsem.at[0]),
        pltpu.make_async_copy(lo_hbm, cf.at[:, 0], lsem.at[1]),
        pltpu.make_async_copy(up_hbm, cf.at[:, 1], lsem.at[2]),
        pltpu.make_async_copy(dg_hbm, av.at[0], lsem.at[3]),
        pltpu.make_async_copy(bl_hbm, av.at[1], lsem.at[4]),
        pltpu.make_async_copy(ab_hbm, av.at[2], lsem.at[5]),
        pltpu.make_async_copy(fb_hbm, fv, lsem.at[6]),
    ]
    for load in loads:
        load.start()

    partners = [dev(o) for o in (-12, -8, -4, -3, -2, -1, 1, 2, 3, 4, 8, 12)]
    partners += [dev(16 * o + c) for o in range(1, 16) for c in (-1, 0, 1)]
    partners += [in_line(o) for o in range(1, 16)]
    barrier = pltpu.get_barrier_semaphore()
    for other in partners:
        pl.semaphore_signal(barrier, inc=1, device_id=(other,), device_id_type=pl.DeviceIdType.MESH)

    def send(src, dst, ssem, rsem, other):
        pltpu.make_async_remote_copy(
            src_ref=src, dst_ref=dst, send_sem=ssem, recv_sem=rsem,
            device_id=(other,), device_id_type=pl.DeviceIdType.MESH,
        ).start()

    def drain(buf, sem):
        pltpu.make_async_copy(buf, buf, sem).wait()

    for load in loads:
        load.wait()

    def send_low(first):
        if first:
            send(cf.at[7], c7.at[1], msend.at[1], mrecv.at[1], dev(-2))
            send(cf.at[7], c7.at[0], msend.at[1], mrecv.at[1], dev(2))
        else:
            send(cf.at[9], c9.at[1], msend.at[2], mrecv.at[2], dev(-8))
            send(cf.at[9], c9.at[0], msend.at[2], mrecv.at[2], dev(8))

    def send_top():
        for p in range(2, 16, 2):
            send(cf.at[11], c11.at[p // 2 - 1], msend.at[3], mrecv.at[3], dev(-16 * p))
        for p in range(4, 16, 4):
            send(cf.at[12], c12.at[p // 4 - 1], msend.at[4], mrecv.at[4], dev(-16 * p))
        send(cf.at[13], c13, msend.at[5], mrecv.at[5], dev(-16 * 8))

    lane = lax.broadcasted_iota(jnp.int32, (8, ROWS), 1)
    sub = lax.broadcasted_iota(jnp.int32, (8, ROWS), 0)
    mine = (lane >= 16 * sub) & (lane < 16 * sub + 16)

    def flag(cond):
        return jnp.where(cond, 1.0, 0.0).astype(F32)

    has_below, has_above = flag(d >= 1), flag(d <= DEV - 2)

    def mul(blocks, v):
        total = blocks[pl.ds(0, 8, stride=8), :] * v[0:1]
        for b in range(1, 8):
            total = total + blocks[pl.ds(b, 8, stride=8), :] * v[b : b + 1]
        return total

    def step(coef, x, below, above):
        return x + mul(coef.at[0], below) + mul(coef.at[1], above)

    def down(u, prev, s):
        return jnp.where(lane < s, pltpu.roll(prev, s, 1), pltpu.roll(u, s, 1))

    def upward(u, following, s):
        return jnp.where(
            lane >= ROWS - s, pltpu.roll(following, ROWS - s, 1), pltpu.roll(u, ROWS - s, 1)
        )

    def far_level(coef, x, below, above, p, by, scale=1, size=DEV):
        place = lax.rem(d + (p % DEV), DEV)
        return step(
            coef, x, below * flag(place >= by), above * flag(place + by <= DEV - 1)
        )

    def send_sums(block, j):
        block = block + pltpu.roll(block, 64, 1)
        block = block + pltpu.roll(block, 32, 1)
        block = block + pltpu.roll(block, 16, 1)
        row = jnp.sum(jnp.where(mine, block, 0.0), axis=0, keepdims=True)
        hz[j, pl.ds(15, 1)] = row
        srcz[j] = row
        for o in range(1, 16):
            send(srcz.at[j], hz.at[j, pl.ds(o - 1, 1)], rsend.at[j, 4], rrecv.at[j, 4], in_line(-o))

    def pass_sums(j):
        drain(hz.at[j, pl.ds(0, 15)], rrecv.at[j, 4])
        row = jnp.sum(hz[j], axis=0, keepdims=True)
        hp[j, pl.ds(15, 1)] = row
        srcp[j] = row
        for o in range(1, 16):
            send(srcp.at[j], hp.at[j, pl.ds(o - 1, 1)], rsend.at[j, 5], rrecv.at[j, 5], dev(-16 * o))

    def take_sums(j):
        drain(hp.at[j, pl.ds(0, 15)], rrecv.at[j, 5])
        total = jnp.sum(hp[j], axis=0, keepdims=True)
        return jnp.sum(jnp.where(mine, total, 0.0), axis=1, keepdims=True) * (1.0 / COUNT) + jnp.zeros((8, ROWS), F32)

    def finish(j, x, hess):
        sums = take_sums(j)
        h = [sums[i : i + 1] for i in range(3)]
        squares = sums[3:4]
        gr[lax.max(j - 1, 0)] = sums
        for i in range(3):
            squares = squares - 2.0 * (h[i] * h[i])
        for c in range(3):
            g = gr[c]
            for i in range(c + 1):
                squares = squares + (1.0 if i == c else 2.0) * (h[c] * h[i]) * g[4 + i : 5 + i]
        length = jnp.sqrt(jnp.maximum(squares, 0.0) + EPS)
        inverse = 1.0 / length
        new = x
        for i in range(3):
            new = new - h[i] * bs[i]
        new = new * inverse
        column = jnp.where(sub < 3, sums, 0.0)
        column = jnp.where(sub == j, length + jnp.zeros((8, ROWS), F32), column)
        hess = jnp.where(lane == j - 1, column, hess)
        return h, inverse, new, hess

    def make_strips(j, f, w):
        low, high, v = f, f, w
        for level in range(NEAR - 1):
            s = 2**level
            low = jnp.where(lane >= 2 * s, pltpu.roll(v, s, 1), low)
            high = jnp.where(lane < ROWS - 2 * s, pltpu.roll(v, ROWS - s, 1), high)
            if level < NEAR - 2:
                v = step(cf.at[level], v, pltpu.roll(v, s, 1), pltpu.roll(v, ROWS - s, 1))
        src1[j, 0] = low
        src1[j, 1] = high

    def ship_strips(j):
        send(src1.at[j, 0], h1.at[j, 1], rsend.at[j, 0], rrecv.at[j, 0], dev(-1))
        send(src1.at[j, 1], h1.at[j, 0], rsend.at[j, 0], rrecv.at[j, 0], dev(1))

    zero = jnp.zeros((8, ROWS), F32)
    for i in range(4):
        bs[i] = zero
    for i in range(3):
        gr[i] = zero
    for i in range(4):
        for c in range(3):
            xs[i, c] = zero

    r = rv[...]
    make_strips(0, r, r)
    wide = lax.broadcasted_iota(jnp.int32, (64, ROWS), 1)

    for which in range(2):
        low = jnp.where(wide < 1, av[1 + which], pltpu.roll(av[0], 1, 1))
        high = jnp.where(wide >= ROWS - 1, av[1 + which], pltpu.roll(av[0], ROWS - 1, 1))
        for level in range(NEAR - 1):
            w = 2 ** (level + 1)
            low = jnp.where(wide >= w, pltpu.roll(cf[level, which], w, 1), low)
            high = jnp.where(wide < ROWS - w, pltpu.roll(cf[level, which], ROWS - w, 1), high)
        packs[0, which] = low
        packs[1, which] = high
    pl.semaphore_wait(barrier, len(partners))
    ship_strips(0)
    send(packs.at[0], got_packs.at[1], msend.at[0], mrecv.at[0], dev(-1))
    send(packs.at[1], got_packs.at[0], msend.at[0], mrecv.at[0], dev(1))
    send_low(True)
    send_sums(jnp.where(sub == 3, jnp.sum(r * r, axis=0, keepdims=True) + zero, 0.0), 0)
    drain(h1.at[0], rrecv.at[0, 0])
    xs[0, 0] = h1[0, 0] * has_below
    xs[0, 1] = r
    xs[0, 2] = h1[0, 1] * has_above
    drain(got_packs, mrecv.at[0])
    for side in range(2):
        for which in range(2):
            pack = got_packs[side, which]
            near_a[side, 1 + which] = pack
            for level in range(NEAR - 1):
                w = 2 ** (level + 1)
                near_c[side, level, which] = pltpu.roll(pack, w if side == 0 else ROWS - w, 1)
        near_a[side, 0] = pltpu.roll(got_packs[side, 0], 1 if side == 0 else ROWS - 1, 1)

    def top_blocks():
        yield 0, 0, cf.at[11]
        yield 1, 0, cf.at[12]
        yield 2, 0, cf.at[13]
        yield 3, 0, cf.at[14]
        yield 2, 8, c13
        for p in range(2, 16, 2):
            yield 0, p, c11.at[p // 2 - 1]
        for p in range(4, 16, 4):
            yield 1, p, c12.at[p // 4 - 1]

    def send_edges():
        for side, row in ((0, 0), (1, ROWS - 1)):
            pack = jnp.where(wide == 33, pltpu.roll(fv[...], (33 - row) % ROWS, 1), 0.0)
            for rank, p, blocks in top_blocks():
                for which in range(2):
                    to = 16 * (2 * rank + which) + p
                    pack = jnp.where(
                        wide == to, pltpu.roll(blocks[which], (to - row) % ROWS, 1), pack
                    )
            edges[side] = pack
        send(edges.at[0], got_edges.at[1], msend.at[6], mrecv.at[6], dev(-1))
        send(edges.at[1], got_edges.at[0], msend.at[6], mrecv.at[6], dev(1))

    def spread(v, index):
        v = jnp.where(index < 16, v, 0.0)
        v = v + pltpu.roll(v, 16, 1)
        v = v + pltpu.roll(v, 32, 1)
        return v + pltpu.roll(v, 64, 1)

    def take_edges():
        drain(got_edges, mrecv.at[6])
        for side in range(2):
            pack = got_edges[side]
            edge_f[side] = pltpu.roll(pack, ROWS - 33, 1)
            for rank in range(4):
                for which in range(2):
                    start = 16 * (2 * rank + which)
                    part = pltpu.roll(pack, ROWS - start, 1) if start else pack
                    edge_c[side, rank, which] = spread(part, wide)

    def edge(side, fields):
        row, c = ((ROWS - 1, -1), (0, 1))[side]
        y = zero
        for p in range(16):
            moved = pltpu.roll(fields[p], (p - row) % ROWS, 1) if p != row else fields[p]
            y = jnp.where(lane == p, moved, y)
        y = spread(y, lane)
        place = lax.rem(d + (c % DEV) + 16 * lax.rem(lane, 16), DEV)
        for rank in range(4):
            by = 2**rank
            below = jnp.where(place >= 16 * by, pltpu.roll(y, by, 1), 0.0)
            above = jnp.where(place + 16 * by <= DEV - 1, pltpu.roll(y, ROWS - by, 1), 0.0)
            y = step(edge_c.at[side, rank], y, below, above)
        return y + mul(edge_f.at[side], y)

    def finish_sums(j, new, hess):
        w = xs[j + 1, 1]
        sums = zero
        rows = [bs[0] * w, bs[1] * w, bs[2] * w, w * w, bs[0] * new, bs[1] * new, bs[2] * new]
        for i, row in enumerate(rows):
            sums = jnp.where(sub == i, jnp.sum(row, axis=0, keepdims=True) + zero, sums)
        send_sums(sums, j + 1)
        return hess

    def body(j, hess, last=False):
        strip = [h1[j, 0] * has_below, h1[j, 1] * has_above]

        def join(left, right, k):
            return (
                jnp.where(lane >= ROWS - k, left, pltpu.roll(strip[0], k, 1)),
                jnp.where(lane < k, right, pltpu.roll(strip[1], ROWS - k, 1)),
            )

        left, right = join(xs[j, 0], xs[j, 2], 1)
        u = [left, xs[j, 1], right]
        for level in range(NEAR):
            s = 2**level
            mid = step(cf.at[level], u[1], down(u[1], u[0], s), upward(u[1], u[2], s))
            if level < NEAR - 1:
                left = step(
                    near_c.at[0, level], u[0], down(u[0], u[0], s), upward(u[0], u[1], s)
                ) * has_below
                right = step(
                    near_c.at[1, level], u[2], down(u[2], u[1], s), upward(u[2], u[2], s)
                ) * has_above
                if level < NEAR - 2:
                    left, right = join(left, right, 2 * s)
                u = [left, mid, right]
            else:
                u = [None, mid, None]
        x = u[1]

        def group(x, src, got, slot, near_coef, level, by, later):
            src[j] = x
            for k, o in enumerate(LOWS):
                send(src.at[j], got.at[j, k], rsend.at[j, slot], rrecv.at[j, slot], dev(-o * by))
            later()
            drain(got.at[j], rrecv.at[j, slot])
            f = {o: got[j, k] for k, o in enumerate(LOWS)}
            f[0] = x
            y = {
                0: far_level(cf.at[level], f[0], f[-1], f[1], 0, by),
                -2: far_level(near_coef.at[0], f[-2], f[-3], f[-1], -2 * by, by),
                2: far_level(near_coef.at[1], f[2], f[1], f[3], 2 * by, by),
            }
            return far_level(cf.at[level + 1], y[0], y[-2], y[2], 0, 2 * by)

        def after_first():
            if not last:

                @pl.when(j == 0)
                def _():
                    send_low(False)
                    send_top()
                    drain(c7, mrecv.at[1])

        def after_second():
            if not last:

                @pl.when(j == 0)
                def _():
                    drain(c9, mrecv.at[2])

                pl.when(j == 1)(take_edges)

        x = group(x, src2, h2, 1, c7, 7, 1, after_first)
        x = group(x, src3, h3, 2, c9, 9, 4, after_second)

        srct[j] = x
        slots = [(0, o) for o in range(1, 16)]
        if last:
            slots += [(c, o) for c in (-1, 1) for o in range(16)]
        got = hm if last else ht.at[j]
        for k, (c, o) in enumerate(slots):
            send(srct.at[j], got.at[k], rsend.at[j, 3], rrecv.at[j, 3], dev(-16 * o - c))
        pass_sums(j)

        if not last:

            @pl.when(j == 0)
            def _():
                drain(c11, mrecv.at[3])
                drain(c12, mrecv.at[4])
                drain(c13, mrecv.at[5])

        drain(got, rrecv.at[j, 3])
        f = [x] + [got[o] for o in range(15)]

        def top(coef, field, p, by):
            return far_level(
                coef, field[p], field[(p - by) % 16], field[(p + by) % 16], 16 * p, 16 * by
            )

        y1 = {p: top(cf.at[11] if p == 0 else c11.at[p // 2 - 1], f, p, 1) for p in range(0, 16, 2)}
        y2 = {p: top(cf.at[12] if p == 0 else c12.at[p // 4 - 1], y1, p, 2) for p in range(0, 16, 4)}
        y3 = {p: top(cf.at[13] if p == 0 else c13, y2, p, 4) for p in (0, 8)}
        x = top(cf.at[14], y3, 0, 8)
        x = x + mul(fv, x)

        h, inverse, new, hess = finish(j, xs[j, 1], hess)
        bs[j] = new
        basis_ref[j] = new

        def operate(coef, c, f, below, above):
            v = 2.0 * f + mul(coef.at[0], f) + mul(coef.at[1], below) + mul(coef.at[2], above)
            for i in range(2):
                v = v - h[i] * xs[i + 1, c]
            return v * inverse

        if last:
            left = edge(0, [got[15 + o] for o in range(16)])
            left = pltpu.roll(left, ROWS - 1, 1) * has_below
            right = edge(1, [got[31 + o] for o in range(16)]) * has_above
            xs[j + 1, 1] = operate(av, 1, x, down(x, left, 1), upward(x, right, 1))
            return finish_sums(j, new, hess)

        make_strips(j + 1, x, operate(av, 1, x, pltpu.roll(x, 1, 1), pltpu.roll(x, ROWS - 1, 1)))
        ship_strips(j + 1)
        pl.when(j == 0)(send_edges)
        drain(h1.at[j + 1], rrecv.at[j + 1, 0])
        left, right = h1[j + 1, 0] * has_below, h1[j + 1, 1] * has_above
        middle = operate(av, 1, x, down(x, left, 1), upward(x, right, 1))
        left = operate(near_a.at[0], 0, left, down(left, left, 1), upward(left, x, 1))
        right = operate(near_a.at[1], 2, right, down(right, x, 1), upward(right, right, 1))
        xs[j + 1, 0] = left * has_below
        xs[j + 1, 1] = middle
        xs[j + 1, 2] = right * has_above

        return finish_sums(j, new, hess)

    hess = lax.fori_loop(0, ITERS - 1, body, zero)
    hess = body(ITERS - 1, hess, True)
    pass_sums(ITERS)
    _, _, new, hess = finish(ITERS, xs[ITERS, 1], hess)
    basis_ref[ITERS] = new
    hess_ref[...] = hess

    drain(packs, msend.at[0])
    drain(edges, msend.at[6])
    drain(c7, msend.at[1])
    drain(c9, msend.at[2])
    drain(c11, msend.at[3])
    drain(c12, msend.at[4])
    drain(c13, msend.at[5])
    for j in range(ITERS + 1):
        drain(hz.at[j, pl.ds(0, 15)], rsend.at[j, 4])
        drain(hp.at[j, pl.ds(0, 15)], rsend.at[j, 5])
        if j < ITERS:
            drain(h1.at[j], rsend.at[j, 0])
            drain(h2.at[j], rsend.at[j, 1])
            drain(h3.at[j], rsend.at[j, 2])
            drain(ht.at[j] if j < 2 else hm, rsend.at[j, 3])


def hand_out(basis_ref, hess_ref, basis_out, hess_out):
    basis_out[...] = basis_ref[...]
    hess_out[...] = hess_ref[: ITERS + 1, :ITERS]


def on_device(right_side, diag_block, below_block, above_block, lower_level, upper_level, final_block):
    block = (64, ROWS)
    tile = (8, ROWS)
    vmem = lambda *lead: pltpu.VMEM(lead, F32)
    basis, hess = pl.pallas_call(
        kernel,
        out_shape=(
            jax.ShapeDtypeStruct((ITERS + 1, 8, ROWS), F32),
            jax.ShapeDtypeStruct(tile, F32),
        ),
        in_specs=[pl.BlockSpec(memory_space=pl.ANY)] * 7,
        out_specs=(pl.BlockSpec(memory_space=pltpu.VMEM), pl.BlockSpec(memory_space=pltpu.VMEM)),
        scratch_shapes=[
            vmem(*tile), vmem(3, *block), vmem(*block), vmem(15, 2, *block),
            vmem(2, 2, *block), vmem(2, 2, *block), vmem(2, 6, 2, *block), vmem(2, 3, *block), vmem(2, 2, *block), vmem(2, 2, *block),
            vmem(7, 2, *block), vmem(3, 2, *block), vmem(2, *block),
            vmem(2, *block), vmem(2, *block), vmem(2, 4, 2, *block), vmem(2, *block),
            vmem(4, 3, *tile), vmem(4, *tile), vmem(3, *tile),
            vmem(4, 2, *tile), vmem(3, *tile), vmem(3, *tile), vmem(3, *tile),
            vmem(4, 1, ROWS), vmem(4, 1, ROWS),
            vmem(3, 2, *tile), vmem(3, 6, *tile), vmem(3, 6, *tile), vmem(2, 15, *tile), vmem(47, *tile),
            vmem(4, 16, ROWS), vmem(4, 16, ROWS),
            pltpu.SemaphoreType.DMA((7,)),
            pltpu.SemaphoreType.DMA((7,)),
            pltpu.SemaphoreType.DMA((7,)),
            pltpu.SemaphoreType.DMA((4, 6)),
            pltpu.SemaphoreType.DMA((4, 6)),
        ],
        compiler_params=pltpu.CompilerParams(collective_id=0, has_side_effects=True),
    )(
        right_side,
        diag_block.reshape(block),
        below_block.reshape(block),
        above_block.reshape(block),
        lower_level.reshape((15,) + block),
        upper_level.reshape((15,) + block),
        final_block.reshape(block),
    )
    return pl.pallas_call(
        hand_out,
        out_shape=(
            jax.ShapeDtypeStruct((ITERS + 1, 8, ROWS), F32),
            jax.ShapeDtypeStruct((ITERS + 1, ITERS), F32),
        ),
        in_specs=[pl.BlockSpec(memory_space=pltpu.VMEM)] * 2,
        out_specs=(pl.BlockSpec(memory_space=pltpu.VMEM), pl.BlockSpec(memory_space=pltpu.VMEM)),
    )(basis, hess)


def solution(mesh):
    blocks = P(None, None, "chain")
    levels = P(None, None, None, "chain")
    return jax.shard_map(
        on_device,
        mesh=mesh,
        in_specs=(P(None, "chain"), blocks, blocks, blocks, levels, levels, blocks),
        out_specs=(P(None, None, "chain"), P()),
        check_vma=False,
    )
```

```python
import functools

import jax
import jax.numpy as jnp
from jax import lax
from jax.experimental import pallas as pl
from jax.experimental.pallas import tpu as pltpu
from jax.sharding import PartitionSpec as P

ITERS = 3
EPS = 1e-06
DEV = 256
ROWS = 128
COUNT = 8 * DEV * ROWS
F32 = jnp.float32
NEAR = 7
LOWS = (-3, -2, -1, 1, 2, 3)


def kernel(
    r_hbm, dg_hbm, bl_hbm, ab_hbm, lo_hbm, up_hbm, fb_hbm,
    basis_ref, hess_ref,
    rv, av, fv, cf,
    packs, got_packs, near_c, near_a, c7, c9, c11, c12, c13,
    edges, got_edges, edge_c, edge_f,
    xs, bs, gr,
    src1, src2, src3, srct, srcz, srcp,
    h1, h2, h3, ht, hm, hz, hp,
    lsem, msend, mrecv, rsend, rrecv,
):
    d = lax.axis_index("chain")
    t = lax.rem(d, 16)
    line = d - t

    def dev(offset):
        return lax.rem(d + (offset % DEV), DEV)

    def in_line(offset):
        return line + lax.rem(t + (offset % 16), 16)

    loads = [
        pltpu.make_async_copy(r_hbm, rv, lsem.at[0]),
        pltpu.make_async_copy(lo_hbm.at[pl.ds(0, 8)], cf.at[pl.ds(0, 8), 0], lsem.at[1]),
        pltpu.make_async_copy(up_hbm.at[pl.ds(0, 8)], cf.at[pl.ds(0, 8), 1], lsem.at[2]),
        pltpu.make_async_copy(dg_hbm, av.at[0], lsem.at[3]),
        pltpu.make_async_copy(bl_hbm, av.at[1], lsem.at[4]),
        pltpu.make_async_copy(ab_hbm, av.at[2], lsem.at[5]),
        pltpu.make_async_copy(fb_hbm, fv, lsem.at[6]),
        pltpu.make_async_copy(lo_hbm.at[pl.ds(8, 7)], cf.at[pl.ds(8, 7), 0], lsem.at[7]),
        pltpu.make_async_copy(up_hbm.at[pl.ds(8, 7)], cf.at[pl.ds(8, 7), 1], lsem.at[8]),
    ]
    for load in loads:
        load.start()

    partners = [dev(o) for o in (-12, -8, -4, -3, -2, -1, 1, 2, 3, 4, 8, 12)]
    partners += [dev(16 * o + c) for o in range(1, 16) for c in (-1, 0, 1)]
    partners += [in_line(o) for o in range(1, 16)]
    barrier = pltpu.get_barrier_semaphore()
    for other in partners:
        pl.semaphore_signal(barrier, inc=1, device_id=(other,), device_id_type=pl.DeviceIdType.MESH)

    def send(src, dst, ssem, rsem, other):
        pltpu.make_async_remote_copy(
            src_ref=src, dst_ref=dst, send_sem=ssem, recv_sem=rsem,
            device_id=(other,), device_id_type=pl.DeviceIdType.MESH,
        ).start()

    def drain(buf, sem):
        pltpu.make_async_copy(buf, buf, sem).wait()

    for load in loads[:6]:
        load.wait()

    def send_low(first):
        if first:
            send(cf.at[7], c7.at[1], msend.at[1], mrecv.at[1], dev(-2))
            send(cf.at[7], c7.at[0], msend.at[1], mrecv.at[1], dev(2))
        else:
            send(cf.at[9], c9.at[1], msend.at[2], mrecv.at[2], dev(-8))
            send(cf.at[9], c9.at[0], msend.at[2], mrecv.at[2], dev(8))

    def send_top():
        for p in range(2, 16, 2):
            send(cf.at[11], c11.at[p // 2 - 1], msend.at[3], mrecv.at[3], dev(-16 * p))
        for p in range(4, 16, 4):
            send(cf.at[12], c12.at[p // 4 - 1], msend.at[4], mrecv.at[4], dev(-16 * p))
        send(cf.at[13], c13, msend.at[5], mrecv.at[5], dev(-16 * 8))

    lane = lax.broadcasted_iota(jnp.int32, (8, ROWS), 1)
    sub = lax.broadcasted_iota(jnp.int32, (8, ROWS), 0)
    mine = (lane >= 16 * sub) & (lane < 16 * sub + 16)

    def flag(cond):
        return jnp.where(cond, 1.0, 0.0).astype(F32)

    has_below, has_above = flag(d >= 1), flag(d <= DEV - 2)

    def mul(blocks, v):
        total = blocks[pl.ds(0, 8, stride=8), :] * v[0:1]
        for b in range(1, 8):
            total = total + blocks[pl.ds(b, 8, stride=8), :] * v[b : b + 1]
        return total

    def step(coef, x, below, above):
        return x + mul(coef.at[0], below) + mul(coef.at[1], above)

    def down(u, prev, s):
        return jnp.where(lane < s, pltpu.roll(prev, s, 1), pltpu.roll(u, s, 1))

    def upward(u, following, s):
        return jnp.where(
            lane >= ROWS - s, pltpu.roll(following, ROWS - s, 1), pltpu.roll(u, ROWS - s, 1)
        )

    def far_level(coef, x, below, above, p, by, scale=1, size=DEV):
        place = lax.rem(d + (p % DEV), DEV)
        return step(
            coef, x, below * flag(place >= by), above * flag(place + by <= DEV - 1)
        )

    def send_sums(block, j):
        block = block + pltpu.roll(block, 64, 1)
        block = block + pltpu.roll(block, 32, 1)
        block = block + pltpu.roll(block, 16, 1)
        row = jnp.sum(jnp.where(mine, block, 0.0), axis=0, keepdims=True)
        hz[j, pl.ds(15, 1)] = row
        srcz[j] = row
        for o in range(1, 16):
            send(srcz.at[j], hz.at[j, pl.ds(o - 1, 1)], rsend.at[j, 4], rrecv.at[j, 4], in_line(-o))

    def pass_sums(j):
        drain(hz.at[j, pl.ds(0, 15)], rrecv.at[j, 4])
        row = jnp.sum(hz[j], axis=0, keepdims=True)
        hp[j, pl.ds(15, 1)] = row
        srcp[j] = row
        for o in range(1, 16):
            send(srcp.at[j], hp.at[j, pl.ds(o - 1, 1)], rsend.at[j, 5], rrecv.at[j, 5], dev(-16 * o))

    def take_sums(j):
        drain(hp.at[j, pl.ds(0, 15)], rrecv.at[j, 5])
        total = jnp.sum(hp[j], axis=0, keepdims=True)
        return jnp.sum(jnp.where(mine, total, 0.0), axis=1, keepdims=True) * (1.0 / COUNT) + jnp.zeros((8, ROWS), F32)

    def finish(j, x, hess):
        sums = take_sums(j)
        h = [sums[i : i + 1] for i in range(3)]
        squares = sums[3:4]
        gr[lax.max(j - 1, 0)] = sums
        for i in range(3):
            squares = squares - 2.0 * (h[i] * h[i])
        for c in range(3):
            g = gr[c]
            for i in range(c + 1):
                squares = squares + (1.0 if i == c else 2.0) * (h[c] * h[i]) * g[4 + i : 5 + i]
        length = jnp.sqrt(jnp.maximum(squares, 0.0) + EPS)
        inverse = 1.0 / length
        new = x
        for i in range(3):
            new = new - h[i] * bs[i]
        new = new * inverse
        column = jnp.where(sub < 3, sums, 0.0)
        column = jnp.where(sub == j, length + jnp.zeros((8, ROWS), F32), column)
        hess = jnp.where(lane == j - 1, column, hess)
        return h, inverse, new, hess

    def make_strips(j, f, w):
        low, high, v = f, f, w
        for level in range(NEAR - 1):
            s = 2**level
            low = jnp.where(lane >= 2 * s, pltpu.roll(v, s, 1), low)
            high = jnp.where(lane < ROWS - 2 * s, pltpu.roll(v, ROWS - s, 1), high)
            if level < NEAR - 2:
                v = step(cf.at[level], v, pltpu.roll(v, s, 1), pltpu.roll(v, ROWS - s, 1))
        src1[j, 0] = low
        src1[j, 1] = high

    def ship_strips(j):
        send(src1.at[j, 0], h1.at[j, 1], rsend.at[j, 0], rrecv.at[j, 0], dev(-1))
        send(src1.at[j, 1], h1.at[j, 0], rsend.at[j, 0], rrecv.at[j, 0], dev(1))

    zero = jnp.zeros((8, ROWS), F32)
    for i in range(4):
        bs[i] = zero
    for i in range(3):
        gr[i] = zero
    for i in range(4):
        for c in range(3):
            xs[i, c] = zero

    r = rv[...]
    wide = lax.broadcasted_iota(jnp.int32, (64, ROWS), 1)

    for which in range(2):
        low = jnp.where(wide < 1, av[1 + which], pltpu.roll(av[0], 1, 1))
        high = jnp.where(wide >= ROWS - 1, av[1 + which], pltpu.roll(av[0], ROWS - 1, 1))
        for level in range(NEAR - 1):
            w = 2 ** (level + 1)
            low = jnp.where(wide >= w, pltpu.roll(cf[level, which], w, 1), low)
            high = jnp.where(wide < ROWS - w, pltpu.roll(cf[level, which], ROWS - w, 1), high)
        packs[0, which] = low
        packs[1, which] = high
    pl.semaphore_wait(barrier, len(partners))
    send(packs.at[0], got_packs.at[1], msend.at[0], mrecv.at[0], dev(-1))
    send(packs.at[1], got_packs.at[0], msend.at[0], mrecv.at[0], dev(1))
    make_strips(0, r, r)
    ship_strips(0)
    send_low(True)
    send_sums(jnp.where(sub == 3, jnp.sum(r * r, axis=0, keepdims=True) + zero, 0.0), 0)
    for load in loads[6:]:
        load.wait()
    drain(h1.at[0], rrecv.at[0, 0])
    xs[0, 0] = h1[0, 0] * has_below
    xs[0, 1] = r
    xs[0, 2] = h1[0, 1] * has_above
    drain(got_packs, mrecv.at[0])
    for side in range(2):
        for which in range(2):
            pack = got_packs[side, which]
            near_a[side, 1 + which] = pack
            for level in range(NEAR - 1):
                w = 2 ** (level + 1)
                near_c[side, level, which] = pltpu.roll(pack, w if side == 0 else ROWS - w, 1)
        near_a[side, 0] = pltpu.roll(got_packs[side, 0], 1 if side == 0 else ROWS - 1, 1)

    def top_blocks():
        yield 0, 0, cf.at[11]
        yield 1, 0, cf.at[12]
        yield 2, 0, cf.at[13]
        yield 3, 0, cf.at[14]
        yield 2, 8, c13
        for p in range(2, 16, 2):
            yield 0, p, c11.at[p // 2 - 1]
        for p in range(4, 16, 4):
            yield 1, p, c12.at[p // 4 - 1]

    def send_edges():
        for side, row in ((0, 0), (1, ROWS - 1)):
            pack = jnp.where(wide == 33, pltpu.roll(fv[...], (33 - row) % ROWS, 1), 0.0)
            for rank, p, blocks in top_blocks():
                for which in range(2):
                    to = 16 * (2 * rank + which) + p
                    pack = jnp.where(
                        wide == to, pltpu.roll(blocks[which], (to - row) % ROWS, 1), pack
                    )
            edges[side] = pack
        send(edges.at[0], got_edges.at[1], msend.at[6], mrecv.at[6], dev(-1))
        send(edges.at[1], got_edges.at[0], msend.at[6], mrecv.at[6], dev(1))

    def spread(v, index):
        v = jnp.where(index < 16, v, 0.0)
        v = v + pltpu.roll(v, 16, 1)
        v = v + pltpu.roll(v, 32, 1)
        return v + pltpu.roll(v, 64, 1)

    def take_edges():
        drain(got_edges, mrecv.at[6])
        for side in range(2):
            pack = got_edges[side]
            edge_f[side] = pltpu.roll(pack, ROWS - 33, 1)
            for rank in range(4):
                for which in range(2):
                    start = 16 * (2 * rank + which)
                    part = pltpu.roll(pack, ROWS - start, 1) if start else pack
                    edge_c[side, rank, which] = spread(part, wide)

    def edge(side, fields):
        row, c = ((ROWS - 1, -1), (0, 1))[side]
        y = zero
        for p in range(16):
            moved = pltpu.roll(fields[p], (p - row) % ROWS, 1) if p != row else fields[p]
            y = jnp.where(lane == p, moved, y)
        y = spread(y, lane)
        place = lax.rem(d + (c % DEV) + 16 * lax.rem(lane, 16), DEV)
        for rank in range(4):
            by = 2**rank
            below = jnp.where(place >= 16 * by, pltpu.roll(y, by, 1), 0.0)
            above = jnp.where(place + 16 * by <= DEV - 1, pltpu.roll(y, ROWS - by, 1), 0.0)
            y = step(edge_c.at[side, rank], y, below, above)
        return y + mul(edge_f.at[side], y)

    def finish_sums(j, new, hess):
        w = xs[j + 1, 1]
        sums = zero
        rows = [bs[0] * w, bs[1] * w, bs[2] * w, w * w, bs[0] * new, bs[1] * new, bs[2] * new]
        for i, row in enumerate(rows):
            sums = jnp.where(sub == i, jnp.sum(row, axis=0, keepdims=True) + zero, sums)
        send_sums(sums, j + 1)
        return hess

    def body(j, hess, last=False):
        strip = [h1[j, 0] * has_below, h1[j, 1] * has_above]

        def join(left, right, k):
            return (
                jnp.where(lane >= ROWS - k, left, pltpu.roll(strip[0], k, 1)),
                jnp.where(lane < k, right, pltpu.roll(strip[1], ROWS - k, 1)),
            )

        left, right = join(xs[j, 0], xs[j, 2], 1)
        u = [left, xs[j, 1], right]
        for level in range(NEAR):
            s = 2**level
            mid = step(cf.at[level], u[1], down(u[1], u[0], s), upward(u[1], u[2], s))
            if level < NEAR - 1:
                left = step(
                    near_c.at[0, level], u[0], down(u[0], u[0], s), upward(u[0], u[1], s)
                ) * has_below
                right = step(
                    near_c.at[1, level], u[2], down(u[2], u[1], s), upward(u[2], u[2], s)
                ) * has_above
                if level < NEAR - 2:
                    left, right = join(left, right, 2 * s)
                u = [left, mid, right]
            else:
                u = [None, mid, None]
        x = u[1]

        def group(x, src, got, slot, near_coef, level, by, later):
            src[j] = x
            for k, o in enumerate(LOWS):
                send(src.at[j], got.at[j, k], rsend.at[j, slot], rrecv.at[j, slot], dev(-o * by))
            later()
            drain(got.at[j], rrecv.at[j, slot])
            f = {o: got[j, k] for k, o in enumerate(LOWS)}
            f[0] = x
            y = {
                0: far_level(cf.at[level], f[0], f[-1], f[1], 0, by),
                -2: far_level(near_coef.at[0], f[-2], f[-3], f[-1], -2 * by, by),
                2: far_level(near_coef.at[1], f[2], f[1], f[3], 2 * by, by),
            }
            return far_level(cf.at[level + 1], y[0], y[-2], y[2], 0, 2 * by)

        def after_first():
            if not last:

                @pl.when(j == 0)
                def _():
                    send_low(False)
                    send_top()
                    drain(c7, mrecv.at[1])

        def after_second():
            pass_sums(j)
            if not last:

                @pl.when(j == 0)
                def _():
                    drain(c9, mrecv.at[2])

                pl.when(j == 1)(take_edges)

        x = group(x, src2, h2, 1, c7, 7, 1, after_first)
        x = group(x, src3, h3, 2, c9, 9, 4, after_second)

        srct[j] = x
        slots = [(0, o) for o in range(1, 16)]
        if last:
            slots += [(c, o) for c in (-1, 1) for o in range(16)]
        got = hm if last else ht.at[j]
        for k, (c, o) in enumerate(slots):
            send(srct.at[j], got.at[k], rsend.at[j, 3], rrecv.at[j, 3], dev(-16 * o - c))
        h, inverse, new, hess = finish(j, xs[j, 1], hess)
        bs[j] = new
        basis_ref[j] = new

        if not last:

            @pl.when(j == 0)
            def _():
                drain(c11, mrecv.at[3])
                drain(c12, mrecv.at[4])
                drain(c13, mrecv.at[5])

        drain(got, rrecv.at[j, 3])
        f = [x] + [got[o] for o in range(15)]

        def top(coef, field, p, by):
            return far_level(
                coef, field[p], field[(p - by) % 16], field[(p + by) % 16], 16 * p, 16 * by
            )

        y1 = {p: top(cf.at[11] if p == 0 else c11.at[p // 2 - 1], f, p, 1) for p in range(0, 16, 2)}
        y2 = {p: top(cf.at[12] if p == 0 else c12.at[p // 4 - 1], y1, p, 2) for p in range(0, 16, 4)}
        y3 = {p: top(cf.at[13] if p == 0 else c13, y2, p, 4) for p in (0, 8)}
        x = top(cf.at[14], y3, 0, 8)
        x = x + mul(fv, x)

        def operate(coef, c, f, below, above):
            v = 2.0 * f + mul(coef.at[0], f) + mul(coef.at[1], below) + mul(coef.at[2], above)
            for i in range(2):
                v = v - h[i] * xs[i + 1, c]
            return v * inverse

        if last:
            left = edge(0, [got[15 + o] for o in range(16)])
            left = pltpu.roll(left, ROWS - 1, 1) * has_below
            right = edge(1, [got[31 + o] for o in range(16)]) * has_above
            xs[j + 1, 1] = operate(av, 1, x, down(x, left, 1), upward(x, right, 1))
            return finish_sums(j, new, hess)

        make_strips(j + 1, x, operate(av, 1, x, pltpu.roll(x, 1, 1), pltpu.roll(x, ROWS - 1, 1)))
        ship_strips(j + 1)
        pl.when(j == 0)(send_edges)
        drain(h1.at[j + 1], rrecv.at[j + 1, 0])
        left, right = h1[j + 1, 0] * has_below, h1[j + 1, 1] * has_above
        middle = operate(av, 1, x, down(x, left, 1), upward(x, right, 1))
        left = operate(near_a.at[0], 0, left, down(left, left, 1), upward(left, x, 1))
        right = operate(near_a.at[1], 2, right, down(right, x, 1), upward(right, right, 1))
        xs[j + 1, 0] = left * has_below
        xs[j + 1, 1] = middle
        xs[j + 1, 2] = right * has_above

        return finish_sums(j, new, hess)

    hess = lax.fori_loop(0, ITERS - 1, body, zero)
    hess = body(ITERS - 1, hess, True)
    pass_sums(ITERS)
    _, _, new, hess = finish(ITERS, xs[ITERS, 1], hess)
    basis_ref[ITERS] = new
    hess_ref[...] = hess

    drain(packs, msend.at[0])
    drain(edges, msend.at[6])
    drain(c7, msend.at[1])
    drain(c9, msend.at[2])
    drain(c11, msend.at[3])
    drain(c12, msend.at[4])
    drain(c13, msend.at[5])
    for j in range(ITERS + 1):
        drain(hz.at[j, pl.ds(0, 15)], rsend.at[j, 4])
        drain(hp.at[j, pl.ds(0, 15)], rsend.at[j, 5])
        if j < ITERS:
            drain(h1.at[j], rsend.at[j, 0])
            drain(h2.at[j], rsend.at[j, 1])
            drain(h3.at[j], rsend.at[j, 2])
            drain(ht.at[j] if j < 2 else hm, rsend.at[j, 3])


def hand_out(basis_ref, hess_ref, basis_out, hess_out):
    basis_out[...] = basis_ref[...]
    hess_out[...] = hess_ref[: ITERS + 1, :ITERS]


def on_device(right_side, diag_block, below_block, above_block, lower_level, upper_level, final_block):
    block = (64, ROWS)
    tile = (8, ROWS)
    vmem = lambda *lead: pltpu.VMEM(lead, F32)
    basis, hess = pl.pallas_call(
        kernel,
        out_shape=(
            jax.ShapeDtypeStruct((ITERS + 1, 8, ROWS), F32),
            jax.ShapeDtypeStruct(tile, F32),
        ),
        in_specs=[pl.BlockSpec(memory_space=pl.ANY)] * 7,
        out_specs=(pl.BlockSpec(memory_space=pltpu.VMEM), pl.BlockSpec(memory_space=pltpu.VMEM)),
        scratch_shapes=[
            vmem(*tile), vmem(3, *block), vmem(*block), vmem(15, 2, *block),
            vmem(2, 2, *block), vmem(2, 2, *block), vmem(2, 6, 2, *block), vmem(2, 3, *block), vmem(2, 2, *block), vmem(2, 2, *block),
            vmem(7, 2, *block), vmem(3, 2, *block), vmem(2, *block),
            vmem(2, *block), vmem(2, *block), vmem(2, 4, 2, *block), vmem(2, *block),
            vmem(4, 3, *tile), vmem(4, *tile), vmem(3, *tile),
            vmem(4, 2, *tile), vmem(3, *tile), vmem(3, *tile), vmem(3, *tile),
            vmem(4, 1, ROWS), vmem(4, 1, ROWS),
            vmem(3, 2, *tile), vmem(3, 6, *tile), vmem(3, 6, *tile), vmem(2, 15, *tile), vmem(47, *tile),
            vmem(4, 16, ROWS), vmem(4, 16, ROWS),
            pltpu.SemaphoreType.DMA((9,)),
            pltpu.SemaphoreType.DMA((7,)),
            pltpu.SemaphoreType.DMA((7,)),
            pltpu.SemaphoreType.DMA((4, 6)),
            pltpu.SemaphoreType.DMA((4, 6)),
        ],
        compiler_params=pltpu.CompilerParams(collective_id=0, has_side_effects=True),
    )(
        right_side,
        diag_block.reshape(block),
        below_block.reshape(block),
        above_block.reshape(block),
        lower_level.reshape((15,) + block),
        upper_level.reshape((15,) + block),
        final_block.reshape(block),
    )
    return pl.pallas_call(
        hand_out,
        out_shape=(
            jax.ShapeDtypeStruct((ITERS + 1, 8, ROWS), F32),
            jax.ShapeDtypeStruct((ITERS + 1, ITERS), F32),
        ),
        in_specs=[pl.BlockSpec(memory_space=pltpu.VMEM)] * 2,
        out_specs=(pl.BlockSpec(memory_space=pltpu.VMEM), pl.BlockSpec(memory_space=pltpu.VMEM)),
    )(basis, hess)


def solution(mesh):
    blocks = P(None, None, "chain")
    levels = P(None, None, None, "chain")
    return jax.shard_map(
        on_device,
        mesh=mesh,
        in_specs=(P(None, "chain"), blocks, blocks, blocks, levels, levels, blocks),
        out_specs=(P(None, None, "chain"), P()),
        check_vma=False,
    )
```

```python
import functools

import jax
import jax.numpy as jnp
from jax import lax
from jax.experimental import pallas as pl
from jax.experimental.pallas import tpu as pltpu
from jax.sharding import PartitionSpec as P

ITERS = 3
EPS = 1e-06
DEV = 256
ROWS = 128
COUNT = 8 * DEV * ROWS
F32 = jnp.float32
NEAR = 7
LOWS = (-3, -2, -1, 1, 2, 3)


def kernel(
    r_hbm, dg_hbm, bl_hbm, ab_hbm, lo_hbm, up_hbm, fb_hbm,
    basis_ref, hess_ref,
    rv, av, fv, cf,
    packs, got_packs, triangle, near_c, near_a, c7, c9, c11, c12, c13,
    edges, got_edges, edge_c, edge_f,
    xs, bs, gr,
    src1, src2, src3, srct, srcz, srcp,
    h1, h2, h3, ht, hm, hz, hp,
    lsem, msend, mrecv, rsend, rrecv,
):
    d = lax.axis_index("chain")
    t = lax.rem(d, 16)
    line = d - t

    def dev(offset):
        return lax.rem(d + (offset % DEV), DEV)

    def in_line(offset):
        return line + lax.rem(t + (offset % 16), 16)

    loads = [
        pltpu.make_async_copy(r_hbm, rv, lsem.at[0]),
        pltpu.make_async_copy(lo_hbm, cf.at[:, 0], lsem.at[1]),
        pltpu.make_async_copy(up_hbm, cf.at[:, 1], lsem.at[2]),
        pltpu.make_async_copy(dg_hbm, av.at[0], lsem.at[3]),
        pltpu.make_async_copy(bl_hbm, av.at[1], lsem.at[4]),
        pltpu.make_async_copy(ab_hbm, av.at[2], lsem.at[5]),
        pltpu.make_async_copy(fb_hbm, fv, lsem.at[6]),
    ]
    for load in loads:
        load.start()

    partners = [dev(o) for o in (-12, -8, -4, -3, -2, -1, 1, 2, 3, 4, 8, 12)]
    partners += [dev(16 * o + c) for o in range(1, 16) for c in (-1, 0, 1)]
    partners += [in_line(o) for o in range(1, 16)]
    barrier = pltpu.get_barrier_semaphore()
    for other in partners:
        pl.semaphore_signal(barrier, inc=1, device_id=(other,), device_id_type=pl.DeviceIdType.MESH)

    def send(src, dst, ssem, rsem, other):
        pltpu.make_async_remote_copy(
            src_ref=src, dst_ref=dst, send_sem=ssem, recv_sem=rsem,
            device_id=(other,), device_id_type=pl.DeviceIdType.MESH,
        ).start()

    def drain(buf, sem):
        pltpu.make_async_copy(buf, buf, sem).wait()

    for load in loads:
        load.wait()

    def send_low(first):
        if first:
            send(cf.at[7], c7.at[1], msend.at[1], mrecv.at[1], dev(-2))
            send(cf.at[7], c7.at[0], msend.at[1], mrecv.at[1], dev(2))
        else:
            send(cf.at[9], c9.at[1], msend.at[2], mrecv.at[2], dev(-8))
            send(cf.at[9], c9.at[0], msend.at[2], mrecv.at[2], dev(8))

    def send_near():
        send(cf.at[pl.ds(0, 6)], near_c.at[1], msend.at[7], mrecv.at[7], dev(-1))
        send(cf.at[pl.ds(0, 6)], near_c.at[0], msend.at[7], mrecv.at[7], dev(1))

    def send_operator():
        send(av, near_a.at[1], msend.at[8], mrecv.at[8], dev(-1))
        send(av, near_a.at[0], msend.at[8], mrecv.at[8], dev(1))

    def send_top():
        for p in range(2, 16, 2):
            send(cf.at[11], c11.at[p // 2 - 1], msend.at[3], mrecv.at[3], dev(-16 * p))
        for p in range(4, 16, 4):
            send(cf.at[12], c12.at[p // 4 - 1], msend.at[4], mrecv.at[4], dev(-16 * p))
        send(cf.at[13], c13, msend.at[5], mrecv.at[5], dev(-16 * 8))

    lane = lax.broadcasted_iota(jnp.int32, (8, ROWS), 1)
    sub = lax.broadcasted_iota(jnp.int32, (8, ROWS), 0)
    mine = (lane >= 16 * sub) & (lane < 16 * sub + 16)

    def flag(cond):
        return jnp.where(cond, 1.0, 0.0).astype(F32)

    has_below, has_above = flag(d >= 1), flag(d <= DEV - 2)

    def mul(blocks, v):
        total = blocks[pl.ds(0, 8, stride=8), :] * v[0:1]
        for b in range(1, 8):
            total = total + blocks[pl.ds(b, 8, stride=8), :] * v[b : b + 1]
        return total

    def step(coef, x, below, above):
        return x + mul(coef.at[0], below) + mul(coef.at[1], above)

    def down(u, prev, s):
        return jnp.where(lane < s, pltpu.roll(prev, s, 1), pltpu.roll(u, s, 1))

    def upward(u, following, s):
        return jnp.where(
            lane >= ROWS - s, pltpu.roll(following, ROWS - s, 1), pltpu.roll(u, ROWS - s, 1)
        )

    def far_level(coef, x, below, above, p, by, scale=1, size=DEV):
        place = lax.rem(d + (p % DEV), DEV)
        return step(
            coef, x, below * flag(place >= by), above * flag(place + by <= DEV - 1)
        )

    def send_sums(block, j):
        block = block + pltpu.roll(block, 64, 1)
        block = block + pltpu.roll(block, 32, 1)
        block = block + pltpu.roll(block, 16, 1)
        row = jnp.sum(jnp.where(mine, block, 0.0), axis=0, keepdims=True)
        hz[j, pl.ds(15, 1)] = row
        srcz[j] = row
        for o in range(1, 16):
            send(srcz.at[j], hz.at[j, pl.ds(o - 1, 1)], rsend.at[j, 4], rrecv.at[j, 4], in_line(-o))

    def pass_sums(j):
        drain(hz.at[j, pl.ds(0, 15)], rrecv.at[j, 4])
        row = jnp.sum(hz[j], axis=0, keepdims=True)
        hp[j, pl.ds(15, 1)] = row
        srcp[j] = row
        for o in range(1, 16):
            send(srcp.at[j], hp.at[j, pl.ds(o - 1, 1)], rsend.at[j, 5], rrecv.at[j, 5], dev(-16 * o))

    def take_sums(j):
        drain(hp.at[j, pl.ds(0, 15)], rrecv.at[j, 5])
        total = jnp.sum(hp[j], axis=0, keepdims=True)
        return jnp.sum(jnp.where(mine, total, 0.0), axis=1, keepdims=True) * (1.0 / COUNT) + jnp.zeros((8, ROWS), F32)

    def finish(j, x, hess):
        sums = take_sums(j)
        h = [sums[i : i + 1] for i in range(3)]
        squares = sums[3:4]
        gr[lax.max(j - 1, 0)] = sums
        for i in range(3):
            squares = squares - 2.0 * (h[i] * h[i])
        for c in range(3):
            g = gr[c]
            for i in range(c + 1):
                squares = squares + (1.0 if i == c else 2.0) * (h[c] * h[i]) * g[4 + i : 5 + i]
        length = jnp.sqrt(jnp.maximum(squares, 0.0) + EPS)
        inverse = 1.0 / length
        new = x
        for i in range(3):
            new = new - h[i] * bs[i]
        new = new * inverse
        column = jnp.where(sub < 3, sums, 0.0)
        column = jnp.where(sub == j, length + jnp.zeros((8, ROWS), F32), column)
        hess = jnp.where(lane == j - 1, column, hess)
        return h, inverse, new, hess

    def make_strips(j, f, w):
        low, high, v = f, f, w
        for level in range(NEAR - 1):
            s = 2**level
            low = jnp.where(lane >= 2 * s, pltpu.roll(v, s, 1), low)
            high = jnp.where(lane < ROWS - 2 * s, pltpu.roll(v, ROWS - s, 1), high)
            if level < NEAR - 2:
                v = step(cf.at[level], v, pltpu.roll(v, s, 1), pltpu.roll(v, ROWS - s, 1))
        src1[j, 0] = low
        src1[j, 1] = high

    def ship_strips(j):
        send(src1.at[j, 0], h1.at[j, 1], rsend.at[j, 0], rrecv.at[j, 0], dev(-1))
        send(src1.at[j, 1], h1.at[j, 0], rsend.at[j, 0], rrecv.at[j, 0], dev(1))

    zero = jnp.zeros((8, ROWS), F32)
    for i in range(4):
        bs[i] = zero
    for i in range(3):
        gr[i] = zero
    for i in range(4):
        for c in range(3):
            xs[i, c] = zero

    r = rv[...]
    make_strips(0, r, r)
    wide = lax.broadcasted_iota(jnp.int32, (64, ROWS), 1)

    for which in range(2):
        low = high = jnp.zeros((64, ROWS), F32)
        for level in range(NEAR - 1):
            w = 2 ** (level + 1)
            low = jnp.where(wide >= w, pltpu.roll(cf[level, which], w, 1), low)
            high = jnp.where(wide < ROWS - w, pltpu.roll(cf[level, which], ROWS - w, 1), high)
        packs[0, which] = low
        packs[1, which] = high
    pl.semaphore_wait(barrier, len(partners))
    ship_strips(0)
    send(packs.at[0], got_packs.at[1], msend.at[0], mrecv.at[0], dev(-1))
    send(packs.at[1], got_packs.at[0], msend.at[0], mrecv.at[0], dev(1))
    send_low(True)
    send_sums(jnp.where(sub == 3, jnp.sum(r * r, axis=0, keepdims=True) + zero, 0.0), 0)
    drain(h1.at[0], rrecv.at[0, 0])
    xs[0, 0] = h1[0, 0] * has_below
    xs[0, 1] = r
    xs[0, 2] = h1[0, 1] * has_above
    drain(got_packs, mrecv.at[0])
    for side in range(2):
        for which in range(2):
            pack = got_packs[side, which]
            for level in range(NEAR - 1):
                w = 2 ** (level + 1)
                triangle[side, level, which] = pltpu.roll(pack, w if side == 0 else ROWS - w, 1)

    def top_blocks():
        yield 0, 0, cf.at[11]
        yield 1, 0, cf.at[12]
        yield 2, 0, cf.at[13]
        yield 3, 0, cf.at[14]
        yield 2, 8, c13
        for p in range(2, 16, 2):
            yield 0, p, c11.at[p // 2 - 1]
        for p in range(4, 16, 4):
            yield 1, p, c12.at[p // 4 - 1]

    def send_edges():
        for side, row in ((0, 0), (1, ROWS - 1)):
            pack = jnp.where(wide == 33, pltpu.roll(fv[...], (33 - row) % ROWS, 1), 0.0)
            for rank, p, blocks in top_blocks():
                for which in range(2):
                    to = 16 * (2 * rank + which) + p
                    pack = jnp.where(
                        wide == to, pltpu.roll(blocks[which], (to - row) % ROWS, 1), pack
                    )
            edges[side] = pack
        send(edges.at[0], got_edges.at[1], msend.at[6], mrecv.at[6], dev(-1))
        send(edges.at[1], got_edges.at[0], msend.at[6], mrecv.at[6], dev(1))

    def spread(v, index):
        v = jnp.where(index < 16, v, 0.0)
        v = v + pltpu.roll(v, 16, 1)
        v = v + pltpu.roll(v, 32, 1)
        return v + pltpu.roll(v, 64, 1)

    def take_edges():
        drain(got_edges, mrecv.at[6])
        for side in range(2):
            pack = got_edges[side]
            edge_f[side] = pltpu.roll(pack, ROWS - 33, 1)
            for rank in range(4):
                for which in range(2):
                    start = 16 * (2 * rank + which)
                    part = pltpu.roll(pack, ROWS - start, 1) if start else pack
                    edge_c[side, rank, which] = spread(part, wide)

    def edge(side, fields):
        row, c = ((ROWS - 1, -1), (0, 1))[side]
        y = zero
        for p in range(16):
            moved = pltpu.roll(fields[p], (p - row) % ROWS, 1) if p != row else fields[p]
            y = jnp.where(lane == p, moved, y)
        y = spread(y, lane)
        place = lax.rem(d + (c % DEV) + 16 * lax.rem(lane, 16), DEV)
        for rank in range(4):
            by = 2**rank
            below = jnp.where(place >= 16 * by, pltpu.roll(y, by, 1), 0.0)
            above = jnp.where(place + 16 * by <= DEV - 1, pltpu.roll(y, ROWS - by, 1), 0.0)
            y = step(edge_c.at[side, rank], y, below, above)
        return y + mul(edge_f.at[side], y)

    def finish_sums(j, new, hess):
        w = xs[j + 1, 1]
        sums = zero
        rows = [bs[0] * w, bs[1] * w, bs[2] * w, w * w, bs[0] * new, bs[1] * new, bs[2] * new]
        for i, row in enumerate(rows):
            sums = jnp.where(sub == i, jnp.sum(row, axis=0, keepdims=True) + zero, sums)
        send_sums(sums, j + 1)
        return hess

    def body(j, hess):
        first, last = j == 0, j == ITERS - 1
        sides = triangle if first else near_c
        def join(left, right, k):
            if not first:
                return left, right
            return (
                jnp.where(lane >= ROWS - k, left, pltpu.roll(xs[0, 0], k, 1)),
                jnp.where(lane < k, right, pltpu.roll(xs[0, 2], ROWS - k, 1)),
            )

        left, right = join(xs[j, 0], xs[j, 2], 1)
        u = [left, xs[j, 1], right]
        for level in range(NEAR):
            s = 2**level
            mid = step(cf.at[level], u[1], down(u[1], u[0], s), upward(u[1], u[2], s))
            if level < NEAR - 1:
                left = step(
                    sides.at[0, level], u[0], down(u[0], u[0], s), upward(u[0], u[1], s)
                ) * has_below
                right = step(
                    sides.at[1, level], u[2], down(u[2], u[1], s), upward(u[2], u[2], s)
                ) * has_above
                if level < NEAR - 2:
                    left, right = join(left, right, 2 * s)
                u = [left, mid, right]
            else:
                u = [None, mid, None]
        x = u[1]

        def group(x, src, got, slot, near_coef, level, by, later):
            src[j] = x
            for k, o in enumerate(LOWS):
                send(src.at[j], got.at[j, k], rsend.at[j, slot], rrecv.at[j, slot], dev(-o * by))
            later()
            drain(got.at[j], rrecv.at[j, slot])
            f = {o: got[j, k] for k, o in enumerate(LOWS)}
            f[0] = x
            y = {
                0: far_level(cf.at[level], f[0], f[-1], f[1], 0, by),
                -2: far_level(near_coef.at[0], f[-2], f[-3], f[-1], -2 * by, by),
                2: far_level(near_coef.at[1], f[2], f[1], f[3], 2 * by, by),
            }
            return far_level(cf.at[level + 1], y[0], y[-2], y[2], 0, 2 * by)

        def after_first():
            if first:
                send_low(False)
                send_top()
                drain(c7, mrecv.at[1])

        def after_second():
            if first:
                pass
                drain(c9, mrecv.at[2])
            elif not last:
                take_edges()

        x = group(x, src2, h2, 1, c7, 7, 1, after_first)
        x = group(x, src3, h3, 2, c9, 9, 4, after_second)

        srct[j] = x
        slots = [(0, o) for o in range(1, 16)]
        if last:
            slots += [(c, o) for c in (-1, 1) for o in range(16)]
        got = hm if last else ht.at[j]
        for k, (c, o) in enumerate(slots):
            send(srct.at[j], got.at[k], rsend.at[j, 3], rrecv.at[j, 3], dev(-16 * o - c))
        pass_sums(j)

        if first:
            send_operator()
            send_near()
            drain(c11, mrecv.at[3])
            drain(c12, mrecv.at[4])
            drain(c13, mrecv.at[5])

        drain(got, rrecv.at[j, 3])
        f = [x] + [got[o] for o in range(15)]

        def top(coef, field, p, by):
            return far_level(
                coef, field[p], field[(p - by) % 16], field[(p + by) % 16], 16 * p, 16 * by
            )

        y1 = {p: top(cf.at[11] if p == 0 else c11.at[p // 2 - 1], f, p, 1) for p in range(0, 16, 2)}
        y2 = {p: top(cf.at[12] if p == 0 else c12.at[p // 4 - 1], y1, p, 2) for p in range(0, 16, 4)}
        y3 = {p: top(cf.at[13] if p == 0 else c13, y2, p, 4) for p in (0, 8)}
        x = top(cf.at[14], y3, 0, 8)
        x = x + mul(fv, x)

        if not last:
            src1[j + 1, 0] = x
            src1[j + 1, 1] = x
            ship_strips(j + 1)
            if first:
                send_edges()

        h, inverse, new, hess = finish(j, xs[j, 1], hess)
        bs[j] = new
        basis_ref[j] = new

        def operate(coef, c, f, below, above):
            v = 2.0 * f + mul(coef.at[0], f) + mul(coef.at[1], below) + mul(coef.at[2], above)
            for i in range(2):
                v = v - h[i] * xs[i + 1, c]
            return v * inverse

        if last:
            left = edge(0, [got[15 + o] for o in range(16)])
            left = pltpu.roll(left, ROWS - 1, 1) * has_below
            right = edge(1, [got[31 + o] for o in range(16)]) * has_above
            xs[j + 1, 1] = operate(av, 1, x, down(x, left, 1), upward(x, right, 1))
            return finish_sums(j, new, hess)

        if first:
            drain(near_a, mrecv.at[8])
            drain(near_c, mrecv.at[7])
        drain(h1.at[j + 1], rrecv.at[j + 1, 0])
        left, right = h1[j + 1, 0] * has_below, h1[j + 1, 1] * has_above
        middle = operate(av, 1, x, down(x, left, 1), upward(x, right, 1))
        left = operate(near_a.at[0], 0, left, down(left, left, 1), upward(left, x, 1))
        right = operate(near_a.at[1], 2, right, down(right, x, 1), upward(right, right, 1))
        xs[j + 1, 0] = left * has_below
        xs[j + 1, 1] = middle
        xs[j + 1, 2] = right * has_above

        return finish_sums(j, new, hess)

    hess = zero
    for j in range(ITERS):
        hess = body(j, hess)
    pass_sums(ITERS)
    _, _, new, hess = finish(ITERS, xs[ITERS, 1], hess)
    basis_ref[ITERS] = new
    hess_ref[...] = hess

    drain(packs, msend.at[0])
    drain(edges, msend.at[6])
    drain(near_c, msend.at[7])
    drain(near_a, msend.at[8])
    drain(c7, msend.at[1])
    drain(c9, msend.at[2])
    drain(c11, msend.at[3])
    drain(c12, msend.at[4])
    drain(c13, msend.at[5])
    for j in range(ITERS + 1):
        drain(hz.at[j, pl.ds(0, 15)], rsend.at[j, 4])
        drain(hp.at[j, pl.ds(0, 15)], rsend.at[j, 5])
        if j < ITERS:
            drain(h1.at[j], rsend.at[j, 0])
            drain(h2.at[j], rsend.at[j, 1])
            drain(h3.at[j], rsend.at[j, 2])
            drain(ht.at[j] if j < 2 else hm, rsend.at[j, 3])


def hand_out(basis_ref, hess_ref, basis_out, hess_out):
    basis_out[...] = basis_ref[...]
    hess_out[...] = hess_ref[: ITERS + 1, :ITERS]


def on_device(right_side, diag_block, below_block, above_block, lower_level, upper_level, final_block):
    block = (64, ROWS)
    tile = (8, ROWS)
    vmem = lambda *lead: pltpu.VMEM(lead, F32)
    basis, hess = pl.pallas_call(
        kernel,
        out_shape=(
            jax.ShapeDtypeStruct((ITERS + 1, 8, ROWS), F32),
            jax.ShapeDtypeStruct(tile, F32),
        ),
        in_specs=[pl.BlockSpec(memory_space=pl.ANY)] * 7,
        out_specs=(pl.BlockSpec(memory_space=pltpu.VMEM), pl.BlockSpec(memory_space=pltpu.VMEM)),
        scratch_shapes=[
            vmem(*tile), vmem(3, *block), vmem(*block), vmem(15, 2, *block),
            vmem(2, 2, *block), vmem(2, 2, *block), vmem(2, 6, 2, *block),
            vmem(2, 6, 2, *block), vmem(2, 3, *block), vmem(2, 2, *block), vmem(2, 2, *block),
            vmem(7, 2, *block), vmem(3, 2, *block), vmem(2, *block),
            vmem(2, *block), vmem(2, *block), vmem(2, 4, 2, *block), vmem(2, *block),
            vmem(4, 3, *tile), vmem(4, *tile), vmem(3, *tile),
            vmem(4, 2, *tile), vmem(3, *tile), vmem(3, *tile), vmem(3, *tile),
            vmem(4, 1, ROWS), vmem(4, 1, ROWS),
            vmem(3, 2, *tile), vmem(3, 6, *tile), vmem(3, 6, *tile), vmem(2, 15, *tile), vmem(47, *tile),
            vmem(4, 16, ROWS), vmem(4, 16, ROWS),
            pltpu.SemaphoreType.DMA((9,)),
            pltpu.SemaphoreType.DMA((9,)),
            pltpu.SemaphoreType.DMA((9,)),
            pltpu.SemaphoreType.DMA((4, 6)),
            pltpu.SemaphoreType.DMA((4, 6)),
        ],
        compiler_params=pltpu.CompilerParams(collective_id=0, has_side_effects=True),
    )(
        right_side,
        diag_block.reshape(block),
        below_block.reshape(block),
        above_block.reshape(block),
        lower_level.reshape((15,) + block),
        upper_level.reshape((15,) + block),
        final_block.reshape(block),
    )
    return pl.pallas_call(
        hand_out,
        out_shape=(
            jax.ShapeDtypeStruct((ITERS + 1, 8, ROWS), F32),
            jax.ShapeDtypeStruct((ITERS + 1, ITERS), F32),
        ),
        in_specs=[pl.BlockSpec(memory_space=pltpu.VMEM)] * 2,
        out_specs=(pl.BlockSpec(memory_space=pltpu.VMEM), pl.BlockSpec(memory_space=pltpu.VMEM)),
    )(basis, hess)


def solution(mesh):
    blocks = P(None, None, "chain")
    levels = P(None, None, None, "chain")
    return jax.shard_map(
        on_device,
        mesh=mesh,
        in_specs=(P(None, "chain"), blocks, blocks, blocks, levels, levels, blocks),
        out_specs=(P(None, None, "chain"), P()),
        check_vma=False,
    )
```
